512 devices in a mesh: groups: 2 (over y), pix: 32 (over z), sub: 4 (over x), rep: 2 (over core).
Axes of the slice: x: 4, y: 2, z: 32, core: 2. Of those that a mesh axis runs over, the one named last changes fastest.
The devices are a block of a 4x8x32 slice.
Arguments:
- gaia_pos: float32 [2, 65536], P(None, ('groups', 'pix', 'sub', 'rep')), parts along dimension 1, may hold values from 0 to 1
- gaia_shape: float32 [2, 65536], P(None, ('groups', 'pix', 'sub', 'rep')), parts along dimension 1, may hold values from 0.15 to 0.6
- gaia_corr: float32 [65536], P(('groups', 'pix', 'sub', 'rep')), parts along dimension 0, may hold values from -0.8 to 0.8
- gaia_dest: int32 [65536, 1], P(('groups', 'pix', 'sub', 'rep')), parts along dimension 0, may hold values from 0 to 127; in each aligned block of 128 rows (0 to 127, 128 to 255, ...) at most 2 rows name the same one
- gaia_cell: int32 [65536], P(('groups', 'pix', 'sub', 'rep')), parts along dimension 0, may hold values from 0 to 127
- wise_pos: float32 [2, 65536], P(None, ('groups', 'pix', 'sub', 'rep')), parts along dimension 1, may hold values from 0 to 1
- wise_shape: float32 [2, 65536], P(None, ('groups', 'pix', 'sub', 'rep')), parts along dimension 1, may hold values from 0.15 to 0.6
- wise_corr: float32 [65536], P(('groups', 'pix', 'sub', 'rep')), parts along dimension 0, may hold values from -0.8 to 0.8
- wise_dest: int32 [65536, 1], P(('groups', 'pix', 'sub', 'rep')), parts along dimension 0, may hold values from 0 to 127; in each aligned block of 128 rows (0 to 127, 128 to 255, ...) at most 2 rows name the same one
- wise_cell: int32 [65536], P(('groups', 'pix', 'sub', 'rep')), parts along dimension 0, may hold values from 0 to 127
Outputs:
- gaia_like: float32 [65536], P(('groups', 'pix', 'sub', 'rep')), parts along dimension 0
- gaia_offset: float32 [2, 65536], P(None, ('groups', 'pix', 'sub', 'rep')), parts along dimension 1
- wise_like: float32 [65536], P(('groups', 'pix', 'sub', 'rep')), parts along dimension 0
The draws below stay inside these ranges and needn't reach their ends.
There are 2 independent parts, one for each index of `groups`. The reference program is written for one: setup_inputs(seed, part) draws one part's arguments, and reference() takes and returns one part's arrays. A program takes and returns all parts, laid end to end along the dimension named above; each array names one. Nothing has to cross between parts.
Inputs may be any that keep to these rules, and one draw needn't show every extreme that they name: `gaia_dest`: among the 128 sources of one device no target appears more than 2 times, and some target appears exactly 2 times; the owner of a source is dest // 4. `wise_dest`: among the 128 sources of one device no target appears more than 2 times, and some target appears exactly 2 times; the owner of a source is dest // 4. `gaia_cell`: pixel row inside the band is cell // 64, column cell % 64. `wise_cell`: pixel row inside the band is cell // 64, column cell % 64.
All inputs are finite; a program needn't handle non-finite values.
Results may differ from the reference program's by a relative error of at most 0.0003.
Values sent between devices are 32-bit elements; how exact they have to be, the bound alone decides.
No kernel may reach another device: no remote copies, remote signals or barrier semaphores. Data moves between devices by JAX's collectives and lax.ppermute only.
A program may use at most 64 MiB of HBM per device.

```python
import math
import jax
import jax.numpy as jnp
import numpy as np
from jax import lax

SRC_DEV = 128
BAND = 2
NCOL = 64
PIX_OWN = 128
DEST = 128
CAP = 2
NG = 32768
N_PIX = 32
N_SUB = 4
N_REP = 2


def touch_ends(values, rng, low, high):
    dims = values.shape
    place = [jax.random.randint(jax.random.fold_in(rng, axis), (), 0, dims[axis]) for axis in range(len(dims))]
    values = values.at[tuple(place)].set(low)
    longest = dims.index(max(dims))
    place[longest] = (place[longest] + 1) % dims[longest]
    return values.at[tuple(place)].set(high)


def steps_of(stream_key, shape, cuts, low, top_value):
    loudness, own = 1.0, jax.random.fold_in(stream_key, 6)
    for dim, blocks in cuts:
        steps = jnp.exp(jax.random.uniform(jax.random.fold_in(own, dim), (blocks,), jnp.float32, low / len(cuts), top_value / len(cuts)))
        loudness = loudness * jnp.repeat(steps, shape[dim] // blocks).reshape([-1 if axis == dim else 1 for axis in range(len(shape))])
    return loudness


def routed_block(key, own, number, rows, count, top, reach, lean):
    ranking = jax.random.permutation(key, count)
    crowded, common = shares(count, rows * top, reach, lean, True), shares(count, rows * top, reach, lean, False)
    places = jnp.arange(count)

    def named(sizes, rotation):
        used = int((sizes > 0).sum())
        fixed = max(1, used // 4)
        shifted = fixed + (places - fixed + rotation * (used - fixed)) % max(1, count - fixed)
        return jnp.zeros((count,), jnp.int32).at[ranking[jnp.where(places < fixed, places, shifted)]].set(jnp.asarray(sizes, jnp.int32))

    sizes = jnp.where(number % 4 == 0, named(crowded, number // 4), named(common, number - number // 4 - 1))
    mixed = jax.random.permutation(jax.random.fold_in(own, 3), count)
    source_of, taker = mixed[0:count // 2 * 2:2], mixed[1:count // 2 * 2:2]
    room = jnp.minimum(sizes[source_of] - 1, reach - sizes[taker]) // 2
    room = jnp.where((source_of == ranking[0]) | (taker == ranking[0]) | (sizes[taker] == 0), 0, jnp.maximum(room, 0))
    shifted = jax.random.randint(jax.random.fold_in(own, 4), (count // 2,), 0, 1 << 20) % (room + 1)
    sizes = sizes.at[source_of].add(-shifted).at[taker].add(shifted)
    labels = jnp.searchsorted(jnp.cumsum(sizes), jnp.arange(rows * top), side="right").astype(jnp.int32)
    grid = labels.reshape(top, rows).T
    grid = grid[jax.random.permutation(jax.random.fold_in(own, 1), rows)]
    rotation = jax.random.randint(jax.random.fold_in(own, 2), (rows, 1), 0, top)
    return jnp.take_along_axis(grid, (jnp.arange(top)[None, :] + rotation) % top, axis=1)


def shares(count, total, bound, lean, full):
    loads = [(1 << 20) // math.isqrt(grade ** lean) + 1 for grade in range(1, count + 1)]
    largest = bound if full else min(bound, max(-(-total // count), total * loads[0] // sum(loads)))
    least = 1 if total - largest >= count - 1 else 0
    given, rest = [largest] + [least] * (count - 1), total - largest - least * (count - 1)
    while rest > 0:
        movable = [i for i in range(1, count) if given[i] < largest] or [i for i in range(1, count) if given[i] < bound]
        whole, left = sum([loads[i] for i in movable]), rest
        for i in movable:
            more = min(bound - given[i], max(1, left * loads[i] // whole), rest)
            given[i] = given[i] + more
            rest = rest - more
    return np.array(given)


def setup_inputs(seed: int = 0, part: int = 0) -> dict:
    key_of = jax.random.split(jax.random.key(seed), 11)
    part_keys = jax.random.split(jax.random.fold_in(key_of[10], part), 11)
    gaia_pos = jnp.clip(1.0 * jax.random.uniform(part_keys[0], (2, NG), jnp.float32) ** steps_of(part_keys[0], (2, NG), ((1, 256),), -0.2, 0.2), 0.0, 1.0)
    gaia_shape = jnp.clip(jnp.exp(math.log(0.6) - 1.3862944 * jax.random.uniform(part_keys[1], (2, NG), jnp.float32) ** steps_of(part_keys[1], (2, NG), ((1, 256),), -0.2, 0.2)), 0.15, 0.6)
    gaia_corr = jnp.clip(jax.random.uniform(part_keys[2], (NG,), jnp.float32, -0.8, 0.8) * steps_of(part_keys[2], (NG,), ((0, 256),), -0.4, 0.0), -0.8, 0.8)
    gaia_dest_keys = jax.random.split(jax.random.fold_in(part_keys[3], 1), NG // SRC_DEV)
    gaia_dest_turns = jax.random.permutation(jax.random.fold_in(part_keys[3], 3), NG // SRC_DEV)
    gaia_dest = jax.vmap(lambda own, number: routed_block(jax.random.fold_in(part_keys[3], 2), own, number, SRC_DEV, DEST, 1, CAP, 2))(gaia_dest_keys, gaia_dest_turns).reshape((NG, 1))
    gaia_cell = touch_ends(jax.random.randint(part_keys[4], (NG,), 0, PIX_OWN), jax.random.fold_in(part_keys[4], 1), 0, PIX_OWN - 1).astype(jnp.int32)
    wise_pos = jnp.clip(1.0 * jax.random.uniform(part_keys[5], (2, NG), jnp.float32) ** steps_of(part_keys[5], (2, NG), ((1, 256),), -0.2, 0.2), 0.0, 1.0)
    wise_shape = jnp.clip(jnp.exp(math.log(0.6) - 1.3862944 * jax.random.uniform(part_keys[6], (2, NG), jnp.float32) ** steps_of(part_keys[6], (2, NG), ((1, 256),), -0.2, 0.2)), 0.15, 0.6)
    wise_corr = jnp.clip(jax.random.uniform(part_keys[7], (NG,), jnp.float32, -0.8, 0.8) * steps_of(part_keys[7], (NG,), ((0, 256),), -0.4, 0.0), -0.8, 0.8)
    wise_dest_keys = jax.random.split(jax.random.fold_in(part_keys[8], 1), NG // SRC_DEV)
    wise_dest_turns = jax.random.permutation(jax.random.fold_in(part_keys[8], 3), NG // SRC_DEV)
    wise_dest = jax.vmap(lambda own, number: routed_block(jax.random.fold_in(part_keys[8], 2), own, number, SRC_DEV, DEST, 1, CAP, 2))(wise_dest_keys, wise_dest_turns).reshape((NG, 1))
    wise_cell = touch_ends(jax.random.randint(part_keys[9], (NG,), 0, PIX_OWN), jax.random.fold_in(part_keys[9], 1), 0, PIX_OWN - 1).astype(jnp.int32)
    return {"gaia_pos": gaia_pos, "gaia_shape": gaia_shape, "gaia_corr": gaia_corr, "gaia_dest": gaia_dest, "gaia_cell": gaia_cell, "wise_pos": wise_pos, "wise_shape": wise_shape, "wise_corr": wise_corr, "wise_dest": wise_dest, "wise_cell": wise_cell}


empty_gaia = -1000.0
empty_wise = -3000.0
row_offset = 4.0
inv_two_pi = 0.15915494309189535

def pack_rows(position, shape, corr, dest, cell, sub_count):
    owner = dest // sub_count
    row = owner * BAND + cell // NCOL
    column = cell % NCOL
    axis_x = shape[0]
    axis_y = shape[1]
    return jnp.stack([position[0], position[1], axis_x * axis_x, axis_y * axis_y, corr * axis_x * axis_y, row.astype(jnp.float32) + row_offset, column.astype(jnp.float32)])

def empty_rows(width, code):
    base = jnp.zeros((7, width), jnp.float32)
    return base.at[2:4].set(1.0).at[5].set(code)

def pair_terms(gaia, wise):
    row_gap = gaia[5][:, None] - wise[5][None, :]
    col_gap = jnp.mod(gaia[6][:, None] - wise[6][None, :] + 1.0, NCOL) - 1.0
    near = (jnp.abs(row_gap) <= 1.0) & (jnp.abs(col_gap) <= 1.0)
    step_x = col_gap + gaia[0][:, None] - wise[0][None, :]
    step_y = row_gap + gaia[1][:, None] - wise[1][None, :]
    spread_x = gaia[2][:, None] + wise[2][None, :]
    spread_y = gaia[3][:, None] + wise[3][None, :]
    spread_xy = gaia[4][:, None] + wise[4][None, :]
    determinant = spread_x * spread_y - spread_xy * spread_xy
    chi_square = (spread_y * step_x * step_x - 2.0 * spread_xy * step_x * step_y + spread_x * step_y * step_y) / determinant
    like = jnp.where(near, jnp.exp(-0.5 * chi_square) * inv_two_pi / jnp.sqrt(determinant), 0.0)
    return (lax.optimization_barrier(jnp.sum(like, axis=1)), lax.optimization_barrier(jnp.sum(like * step_x, axis=1)), lax.optimization_barrier(jnp.sum(like * step_y, axis=1)), lax.optimization_barrier(jnp.sum(like, axis=0)))

def slot_numbers(dest):
    per_device = dest.reshape(-1, SRC_DEV)
    order = jnp.arange(SRC_DEV, dtype=jnp.int32)

    def ranks(line):
        same = (line[:, None] == line[None, :]) & (order[None, :] < order[:, None])
        return lax.optimization_barrier(jnp.sum(same.astype(jnp.int32), axis=1, dtype=jnp.int32))
    rank = lax.map(ranks, per_device)
    device = jnp.arange(per_device.shape[0], dtype=jnp.int32)[:, None]
    source_group = device // N_REP
    replica = device % N_REP
    slot = ((per_device * N_REP + replica) * DEST + source_group) * CAP + rank
    return slot.reshape(-1).astype(jnp.int32)

def reference(gaia_pos, gaia_shape, gaia_corr, gaia_dest, gaia_cell, wise_pos, wise_shape, wise_corr, wise_dest, wise_cell):
    received = DEST * CAP
    block = N_SUB * N_REP * received
    whole = N_PIX * block
    width = received // 2
    gaia_rows = pack_rows(gaia_pos, gaia_shape, gaia_corr, gaia_dest[:, 0], gaia_cell, N_SUB)
    wise_rows = pack_rows(wise_pos, wise_shape, wise_corr, wise_dest[:, 0], wise_cell, N_SUB)
    gaia_slot = slot_numbers(gaia_dest[:, 0])
    wise_slot = slot_numbers(wise_dest[:, 0])
    gaia_all = empty_rows(whole, empty_gaia).at[:, gaia_slot].set(gaia_rows)
    wise_all = empty_rows(whole, empty_wise).at[:, wise_slot].set(wise_rows)
    padding = jnp.zeros((7, block), jnp.float32)
    wise_all = jnp.concatenate([padding, wise_all, padding], axis=1)

    def owner_step(wise_total, owner):
        start = (owner * block).astype(jnp.int32)
        gaia = lax.dynamic_slice_in_dim(gaia_all, start, block, 1)
        nearby = lax.dynamic_slice_in_dim(wise_all, start, 3 * block, 1)
        pieces = nearby.reshape(7, -1, width).transpose(1, 0, 2)

        def column_step(totals, piece):
            like, moment_x, moment_y, column_sums = pair_terms(gaia, piece)
            return (totals + jnp.stack([like, moment_x, moment_y]), column_sums)
        totals, column_sums = lax.scan(column_step, jnp.zeros((3, block), jnp.float32), pieces)
        part = lax.dynamic_slice_in_dim(wise_total, start, 3 * block, 0) + column_sums.reshape(-1)
        wise_total = lax.dynamic_update_slice_in_dim(wise_total, part, start, 0)
        return (wise_total, totals)
    wise_total, gaia_blocks = lax.scan(owner_step, jnp.zeros(((N_PIX + 2) * block,), jnp.float32), jnp.arange(N_PIX, dtype=jnp.int32))
    gaia_flat = gaia_blocks.transpose(1, 0, 2).reshape(3, -1)
    wise_flat = wise_total[block:block + whole]
    return (gaia_flat[0][gaia_slot], gaia_flat[1:3][:, gaia_slot], wise_flat[wise_slot])
```

```python
import math

import jax
import jax.numpy as jnp
from jax import lax
from jax.experimental import pallas as pl
from jax.experimental.pallas import tpu as pltpu
from jax.sharding import PartitionSpec as P

NCOL = 64
CAP = 2
LANES = 128
SLOT_LANES = 16
FIELDS = 8
EMPTY_BIT = 4096
ROW_BIT = 8192
LAMBDA = 2.0 * math.log(2.0)
GAIN = LAMBDA / (2.0 * math.pi)
GROUPS = 4
USED = 6
INTERPRET = False

f32 = jnp.float32
bf16 = jnp.bfloat16
i32 = jnp.int32


def iota(shape, dim):
    return lax.broadcasted_iota(i32, shape, dim)


def split3(x):
    high = x.astype(bf16)
    rest = x - high.astype(f32)
    middle = rest.astype(bf16)
    low = (rest - middle.astype(f32)).astype(bf16)
    return high, middle, low


def dot(a, b, contract):
    return lax.dot_general(a, b, (contract, ((), ())), preferred_element_type=f32)


def one_hot(mask):
    return jnp.where(mask, 1.0, 0.0).astype(bf16)


def call(body, outs, scratch=()):
    return pl.pallas_call(
        body,
        out_shape=outs,
        scratch_shapes=list(scratch),
        compiler_params=pltpu.CompilerParams(vmem_limit_bytes=8 << 20),
        interpret=INTERPRET,
    )


def owners_and_ranks(dest_g, dest_w, sub_count):
    n = dest_g.shape[1]
    shift = sub_count.bit_length() - 1
    own_g, own_w = dest_g >> shift, dest_w >> shift
    both = jnp.concatenate([own_g.astype(f32), own_w.astype(f32), jnp.zeros((6, n), f32)], axis=0)
    columns = jnp.transpose(both)
    earlier = iota((n, n), 0) < iota((n, n), 1)

    def rank(row, column):
        same = (row.astype(f32) == column) & earlier
        return jnp.sum(jnp.where(same, 1.0, 0.0), axis=0, keepdims=True).astype(i32)

    return own_g, own_w, rank(own_g, columns[:, 0:1]), rank(own_w, columns[:, 1:2])


def send_body(pix_count, sub_count):
    slots = CAP * sub_count

    def body(gp, gs, gc, gd, gl, wp, ws, wc, wd, wl, msg):
        n = gp.shape[1]
        own_g, own_w, rank_g, rank_w = owners_and_ranks(gd[...], wd[...], sub_count)

        def fields(pos, shape, corr, cell):
            a, b = shape[0:1, :], shape[1:2, :]
            return jnp.concatenate(
                [
                    pos[0:1, :],
                    pos[1:2, :],
                    (a * a) * LAMBDA,
                    (b * b) * LAMBDA,
                    ((corr * a) * b) * (2.0 * LAMBDA),
                    cell.astype(f32) + 1.0,
                    jnp.zeros((2, n), f32),
                ],
                axis=0,
            )

        data_g = fields(gp, gs, gc[...], gl[...])
        data_w = fields(wp, ws, wc[...], wl[...])
        zero = jnp.zeros((FIELDS, n), f32)
        left, right = [], []
        for s in range(slots):
            left += [jnp.where(rank_g == s, data_g, 0.0), zero]
            right += [zero, jnp.where(rank_w == s, data_w, 0.0)]
        table = jnp.concatenate([jnp.concatenate(left, axis=0), jnp.concatenate(right, axis=0)], axis=1)
        rows = 3 * pix_count
        r = iota((rows, 2 * n), 0)
        target = jnp.floor((r.astype(f32) + 0.5) * (1.0 / 3.0)).astype(i32)
        side = r - 3 * target
        owner = jnp.concatenate([own_g, own_w], axis=1)
        upper = jnp.concatenate([gl[...], wl[...]], axis=1) >> (NCOL.bit_length() - 1)
        wanted = (owner == target + side - 1) & ((side == 1) | (upper == jnp.where(side == 0, 1, 0)))
        pick = one_hot(wanted)
        msg[...] = sum(dot(pick, part, ((1,), (1,))) for part in split3(table))

    return body


def compact_body(pix_count, slots, members, width):
    own_lanes = pix_count

    def body(got, out, own, ranks, chunk):
        lanes = 3 * pix_count
        parts = [got[pl.ds(j, pix_count, stride=3), :] for j in (1, 0, 2)]
        parts.append(jnp.zeros((LANES - lanes, LANES), f32))
        data = jnp.transpose(jnp.concatenate(parts, axis=0))
        lane8 = iota((FIELDS, LANES), 1)
        row8 = iota((FIELDS, LANES), 0)
        is_own = lane8 < own_lanes
        is_low = (lane8 >= own_lanes) & (lane8 < 2 * own_lanes)
        before = one_hot(iota((LANES, LANES), 0) < iota((LANES, LANES), 1))
        below = one_hot(iota((slots, slots), 1) < iota((slots, slots), 0))
        chunk[...] = jnp.zeros(chunk.shape, f32)
        rank_rows = []
        for c in range(2):
            pieces, codes = [], []
            for s in range(slots):
                x = data[s * SLOT_LANES + c * FIELDS : s * SLOT_LANES + (c + 1) * FIELDS, :]
                code = x[5:6, :]
                filled = code > 0.5
                cell = code.astype(i32) - 1
                row = jnp.where(is_own, cell >> 6, jnp.where(is_low, -1, 2)).astype(f32)
                away = jnp.where(is_own, 0, jnp.where(is_low, 512, 256))
                own_row = jnp.where(is_own, (cell >> 6) * ROW_BIT, 0)
                seen = ((cell & (NCOL - 1)) - away + EMPTY_BIT + own_row).astype(f32)
                x = jnp.where(row8 == 1, x + row, jnp.where(row8 == 5, seen, x))
                pieces.append(jnp.where(filled, x, 0.0))
                codes.append(code)
            filled = jnp.concatenate(codes, axis=0) > 0.5
            flag_own = jnp.where(filled & (iota((slots, LANES), 1) < own_lanes), 1.0, 0.0)
            flag_far = jnp.where(filled & (iota((slots, LANES), 1) >= own_lanes), 1.0, 0.0)

            def places(flag):
                inside = dot(flag.astype(bf16), before, ((1,), (0,)))
                totals = jnp.broadcast_to(jnp.sum(flag, axis=1, keepdims=True), (slots, LANES))
                ahead = dot(below, totals.astype(bf16), ((1,), (0,)))
                return inside + ahead, jnp.sum(totals, axis=0, keepdims=True)

            place_own, count_own = places(flag_own)
            place_far, count_far = places(flag_far)
            place = jnp.where(flag_own > 0.5, place_own, place_far + count_own)
            place = jnp.where(filled, place, -1.0)
            count = count_own + count_far
            rank_rows.append(place)
            stacked = [jnp.concatenate(split3(p), axis=0) for p in pieces]
            total = jnp.max(count)
            for t in range(width // LANES):

                @pl.when(total > t * LANES)
                def _(t=t, c=c, place=place, stacked=stacked, count=count, count_own=count_own):
                    goal = iota((LANES, LANES), 0).astype(f32) + float(t * LANES)
                    acc = jnp.zeros((3 * FIELDS, LANES), f32)
                    for s in range(slots):
                        pick = one_hot(goal == place[s : s + 1, :])
                        acc = acc + dot(stacked[s], pick, ((1,), (1,)))
                    x = acc[0:8, :] + acc[8:16, :] + acc[16:24, :]
                    x = jnp.where(row8 == 6, count, jnp.where(row8 == 7, count_own, x))
                    chunk[c * FIELDS : (c + 1) * FIELDS, t * LANES : (t + 1) * LANES] = x

        ranks[...] = jnp.transpose(jnp.concatenate(rank_rows + [jnp.zeros((LANES - 2 * slots, LANES), f32)], axis=0))
        value = chunk[...]
        own[...] = value[:, : own.shape[1]]
        for d in range(members):
            out[d] = value

    return body


def match_body(pix_count, slots, members, width):
    block = 8 * GROUPS
    used = 2 * USED
    early = 5 * block

    def body(near, own, ranks, out, wide, line, totals):
        own_width = pix_count * slots
        lane8 = iota((8, LANES), 1)
        stacked = jnp.concatenate([p.astype(f32) for p in split3(own[...])], axis=0)
        columns = jnp.transpose(stacked).astype(bf16)
        spread_to = iota((6 * FIELDS, used * LANES), 1) >> 7
        field_of = spread_to + jnp.where(spread_to >= USED, FIELDS - USED, 0)
        spread = one_hot((iota((6 * FIELDS, used * LANES), 0) & (2 * FIELDS - 1)) == field_of)
        wide[0:early, :] = dot(columns[0:early, :], spread, ((1,), (0,)))
        count_own = [jnp.max(own[c * FIELDS + 7 : c * FIELDS + 8, 0:LANES]).astype(i32) for c in range(2)]

        @pl.when(jnp.maximum(count_own[0], count_own[1]) > early)
        def _():
            wide[early:own_width, :] = dot(columns[early:own_width, :], spread, ((1,), (0,)))

        counts = [
            [jnp.max(near[d, c * FIELDS + 6 : c * FIELDS + 7, 0:LANES]).astype(i32) for d in range(members)] for c in range(2)
        ]
        ends = []
        for c in range(2):
            start = jnp.int32(0)
            for d in range(members):
                shift = start & (LANES - 1)
                base = start >> 7
                keep = lane8 >= shift

                def put(k, x, c=c, base=base):
                    line[c, base + k] = x

                def turned(k, c=c, d=d, shift=shift):
                    return pltpu.roll(near[d, c * FIELDS : (c + 1) * FIELDS, k * LANES : (k + 1) * LANES], shift, 1)

                last = jnp.zeros((FIELDS, LANES), f32) if d == 0 else line[c, base]
                for k in range(3):
                    now = turned(k)
                    put(k, jnp.where(keep, now, last))
                    last = now
                put(3, jnp.where(keep, 0.0, last))
                put(4, jnp.zeros((FIELDS, LANES), f32))

                @pl.when(counts[c][d] > 3 * LANES)
                def _(c=c, base=base, keep=keep, put=put, turned=turned):
                    last = line[c, base + 3]
                    for k in range(3, width // LANES):
                        now = turned(k)
                        put(k, jnp.where(keep, now, last))
                        last = now
                    put(width // LANES, jnp.where(keep, 0.0, last))
                    put(width // LANES + 1, jnp.zeros((FIELDS, LANES), f32))

                start = start + counts[c][d]
            ends.append(lax.div(start + (2 * LANES - 1), 2 * LANES))

        for c in range(2):
            other = 1 - c
            blocks = lax.div(count_own[c] + (block - 1), block)

            def own_block(b, _, c=c, other=other):
                base = pl.multiple_of(b * block, 8)
                fields = []
                for g in range(GROUPS):
                    col = [wide[pl.ds(base + 8 * g, 8), (c * USED + f) * LANES : (c * USED + f + 1) * LANES] for f in range(USED)]
                    code = col[5].astype(i32)
                    own_code = code + (NCOL + 1 - EMPTY_BIT)
                    mask = jnp.where(code < ROW_BIT, 256, 512) | (EMPTY_BIT | (NCOL - 1))
                    fields.append((col[0] - 1.0, col[1], col[2], col[3], col[4], own_code, mask))

                def pairs(t, acc):
                    acc = [list(a) for a in acc]
                    for half in range(2):
                        at = line.at[other, 2 * t + half]
                        row = [jnp.broadcast_to(at[f : f + 1, :], (8, LANES)) for f in range(USED)]
                        code = row[5].astype(i32) - EMPTY_BIT
                        for g in range(GROUPS):
                            px, py, xx, yy, xy, own_code, mask = fields[g]
                            step = (own_code - code) & mask
                            dx = step.astype(f32) + (px - row[0])
                            dy = py - row[1]
                            sx, sy, sxy = xx + row[2], yy + row[3], xy + row[4]
                            det = sx * sy - 0.25 * (sxy * sxy)
                            root = lax.rsqrt(det)
                            chi = dy * (sxy * dx - sx * dy) - sy * (dx * dx)
                            like = jnp.exp2(chi * (root * root)) * root
                            like = jnp.where(step <= 2, like, 0.0)
                            acc[g][0] = acc[g][0] + like
                            if c == 0:
                                acc[g][1] = acc[g][1] + like * dx
                                acc[g][2] = acc[g][2] + like * dy
                    return tuple(tuple(a) for a in acc)

                zero = jnp.zeros((8, LANES), f32)
                acc = tuple((zero,) * (3 if c == 0 else 1) for _ in range(GROUPS))
                acc = lax.fori_loop(0, ends[other], pairs, acc)
                for g in range(GROUPS):
                    for k, a in enumerate(acc[g]):
                        totals[3 * c + k, pl.ds(base + 8 * g, 8), :] = a
                return 0

            lax.fori_loop(0, blocks, own_block, 0)

        f_of_lane = lane8 & (SLOT_LANES - 1)
        goal = iota((pix_count, own_width), 1).astype(f32)
        picks, values = [], []
        for c in range(2):
            columns = [ranks[0:pix_count, c * slots + s : c * slots + s + 1] for s in range(slots)]
            picks.append(jnp.concatenate([one_hot(r == goal) for r in columns], axis=0))
            rows = []
            for g in range(own_width // 8):
                live = (iota((8, LANES), 0) + 8 * g) < count_own[c]
                value = jnp.zeros((8, LANES), f32)
                for k in range(3 if c == 0 else 1):
                    total = jnp.sum(totals[3 * c + k, 8 * g : 8 * g + 8, :], axis=1, keepdims=True) * GAIN
                    value = jnp.where(f_of_lane == c * FIELDS + k, total, value)
                rows.append(jnp.where(live, value, 0.0))
            values.append(jnp.concatenate(rows, axis=0))
        pick = jnp.concatenate(picks, axis=1)
        result = sum(dot(pick, part, ((1,), (0,))) for part in split3(jnp.concatenate(values, axis=0)))
        slot_of_lane = iota((pix_count, LANES), 1) >> 4
        final = jnp.zeros((pix_count, LANES), f32)
        for s in range(slots):
            final = final + jnp.where(slot_of_lane == s, result[s * pix_count : (s + 1) * pix_count, :], 0.0)
        out[...] = final

    return body


def return_body(pix_count, sub_count):
    slots = CAP * sub_count

    def body(back, gd, wd, like, offset, wise):
        n = gd.shape[1]
        own_g, own_w, rank_g, rank_w = owners_and_ranks(gd[...], wd[...], sub_count)
        owner = jnp.concatenate([own_g, own_w], axis=1)
        pick = one_hot(iota((pix_count, 2 * n), 0) == owner)
        turned = jnp.transpose(back[...])
        found = sum(dot(part, pick, ((1,), (0,))) for part in split3(turned))
        gaia = jnp.zeros((FIELDS, n), f32)
        other = jnp.zeros((FIELDS, n), f32)
        for s in range(slots):
            at = s * SLOT_LANES
            gaia = gaia + jnp.where(rank_g == s, found[at : at + FIELDS, 0:n], 0.0)
            other = other + jnp.where(rank_w == s, found[at + FIELDS : at + 2 * FIELDS, n : 2 * n], 0.0)
        like[...] = gaia[0:1, :]
        offset[...] = gaia[1:3, :]
        wise[...] = other[0:1, :]

    return body


def stages(pix_count, sub_count, members, n):
    slots = CAP * sub_count
    width = 3 * pix_count * slots
    own_width = pix_count * slots
    send = call(send_body(pix_count, sub_count), jax.ShapeDtypeStruct((3 * pix_count, LANES), f32))
    compact = call(
        compact_body(pix_count, slots, members, width),
        (
            jax.ShapeDtypeStruct((members, 2 * FIELDS, width), f32),
            jax.ShapeDtypeStruct((2 * FIELDS, own_width), f32),
            jax.ShapeDtypeStruct((LANES, LANES), f32),
        ),
        [pltpu.VMEM((2 * FIELDS, width), f32)],
    )
    match = call(
        match_body(pix_count, slots, members, width),
        jax.ShapeDtypeStruct((pix_count, LANES), f32),
        [
            pltpu.VMEM((own_width, 2 * USED * LANES), f32),
            pltpu.VMEM((2, members * width // LANES + 8, FIELDS, LANES), f32),
            pltpu.VMEM((4, own_width, LANES), f32),
        ],
    )
    back = call(
        return_body(pix_count, sub_count),
        (
            jax.ShapeDtypeStruct((1, n), f32),
            jax.ShapeDtypeStruct((2, n), f32),
            jax.ShapeDtypeStruct((1, n), f32),
        ),
    )
    return send, compact, match, back


def shards(gaia_pos, gaia_shape, gaia_corr, gaia_dest, gaia_cell, wise_pos, wise_shape, wise_corr, wise_dest, wise_cell):
    pix_count = lax.axis_size("pix")
    sub_count = lax.axis_size("sub")
    members = sub_count * lax.axis_size("rep")
    n = gaia_pos.shape[1]
    send, compact, match, back = stages(pix_count, sub_count, members, n)
    row = lambda x: x.reshape(1, n)
    gd, wd = row(gaia_dest), row(wise_dest)
    msg = send(gaia_pos, gaia_shape, row(gaia_corr), gd, row(gaia_cell), wise_pos, wise_shape, row(wise_corr), wd, row(wise_cell))
    got = lax.all_to_all(msg.reshape(pix_count, 1, 3 * LANES), "pix", 0, 0, tiled=True)
    chunks, own, ranks = compact(got.reshape(3 * pix_count, LANES))
    near = lax.all_to_all(chunks, ("sub", "rep"), 0, 0, tiled=True)
    results = match(near, own, ranks)
    returned = lax.all_to_all(results.reshape(pix_count, 1, LANES), "pix", 0, 0, tiled=True)
    like, offset, wise = back(returned.reshape(pix_count, LANES), gd, wd)
    return like.reshape(n), offset, wise.reshape(n)


def solution(mesh):
    flat = P(("groups", "pix", "sub", "rep"))
    pair = P(None, ("groups", "pix", "sub", "rep"))
    column = P(("groups", "pix", "sub", "rep"), None)
    return jax.shard_map(
        shards,
        mesh=mesh,
        in_specs=(pair, pair, flat, column, flat, pair, pair, flat, column, flat),
        out_specs=(flat, pair, flat),
        check_vma=False,
    )
```

```python
import math

import jax
import jax.numpy as jnp
from jax import lax
from jax.experimental import pallas as pl
from jax.experimental.pallas import tpu as pltpu
from jax.sharding import PartitionSpec as P

NCOL = 64
CAP = 2
LANES = 128
SLOT_LANES = 16
FIELDS = 8
EMPTY_BIT = 4096
ROW_BIT = 8192
LAMBDA = 2.0 * math.log(2.0)
GAIN = LAMBDA / (2.0 * math.pi)
GROUPS = 4
USED = 6
INTERPRET = False

f32 = jnp.float32
bf16 = jnp.bfloat16
i32 = jnp.int32


def iota(shape, dim):
    return lax.broadcasted_iota(i32, shape, dim)


def split3(x):
    high = x.astype(bf16)
    rest = x - high.astype(f32)
    middle = rest.astype(bf16)
    low = (rest - middle.astype(f32)).astype(bf16)
    return high, middle, low


def dot(a, b, contract):
    return lax.dot_general(a, b, (contract, ((), ())), preferred_element_type=f32)


def one_hot(mask):
    return jnp.where(mask, 1.0, 0.0).astype(bf16)


def call(body, outs, scratch=()):
    return pl.pallas_call(
        body,
        out_shape=outs,
        scratch_shapes=list(scratch),
        compiler_params=pltpu.CompilerParams(vmem_limit_bytes=16 << 20),
        interpret=INTERPRET,
    )


def first_peer(pix_count, peers):
    return peers - pix_count // 2


def message_rows(width):
    return width // LANES * 2 * USED + FIELDS


def owners_and_ranks(dest_g, dest_w, sub_count):
    n = dest_g.shape[1]
    shift = sub_count.bit_length() - 1
    own_g, own_w = dest_g >> shift, dest_w >> shift
    both = jnp.concatenate([own_g.astype(f32), own_w.astype(f32), jnp.zeros((6, n), f32)], axis=0)
    columns = jnp.transpose(both)
    earlier = iota((n, n), 0) < iota((n, n), 1)

    def rank(row, column):
        same = (row.astype(f32) == column) & earlier
        return jnp.sum(jnp.where(same, 1.0, 0.0), axis=0, keepdims=True).astype(i32)

    return own_g, own_w, rank(own_g, columns[:, 0:1]), rank(own_w, columns[:, 1:2])


def send_body(pix_count, sub_count, peers):
    slots = CAP * sub_count
    turn = first_peer(pix_count, peers)

    def body(gp, gs, gc, gd, gl, wp, ws, wc, wd, wl, msg):
        n = gp.shape[1]
        own_g, own_w, rank_g, rank_w = owners_and_ranks(gd[...], wd[...], sub_count)

        def fields(pos, shape, corr, cell):
            a, b = shape[0:1, :], shape[1:2, :]
            return jnp.concatenate(
                [
                    pos[0:1, :],
                    pos[1:2, :],
                    (a * a) * LAMBDA,
                    (b * b) * LAMBDA,
                    ((corr * a) * b) * (2.0 * LAMBDA),
                    cell.astype(f32) + 1.0,
                    jnp.zeros((2, n), f32),
                ],
                axis=0,
            )

        data_g = fields(gp, gs, gc[...], gl[...])
        data_w = fields(wp, ws, wc[...], wl[...])
        zero = jnp.zeros((FIELDS, n), f32)
        left, right = [], []
        for s in range(slots):
            left += [jnp.where(rank_g == s, data_g, 0.0), zero]
            right += [zero, jnp.where(rank_w == s, data_w, 0.0)]
        table = jnp.concatenate([jnp.concatenate(left, axis=0), jnp.concatenate(right, axis=0)], axis=1)
        rows = 3 * peers
        r = iota((rows, 2 * n), 0)
        peer = jnp.floor((r.astype(f32) + 0.5) * (1.0 / 3.0)).astype(i32)
        side = r - 3 * peer
        band = (peer - turn) & (peers - 1)
        owner = jnp.concatenate([own_g, own_w], axis=1)
        upper = jnp.concatenate([gl[...], wl[...]], axis=1) >> (NCOL.bit_length() - 1)
        edge = (side == 1) | (upper == jnp.where(side == 0, 1, 0))
        pick = one_hot((owner == band + side - 1) & (band < pix_count) & edge)
        msg[...] = sum(dot(pick, part, ((1,), (1,))) for part in split3(table))

    return body


def compact_body(peers, slots, members, width):
    lanes = -(-3 * peers // LANES) * LANES
    tiles = width // LANES

    def body(got, out, own, ranks, chunk):
        parts = [got[pl.ds(j, peers, stride=3), :] for j in (1, 0, 2)]
        parts.append(jnp.zeros((lanes - 3 * peers, LANES), f32))
        data = jnp.transpose(jnp.concatenate(parts, axis=0))
        lane8 = iota((FIELDS, lanes), 1)
        row8 = iota((FIELDS, lanes), 0)
        row_of = iota((FIELDS, LANES), 0)
        is_own = lane8 < peers
        is_low = (lane8 >= peers) & (lane8 < 2 * peers)
        before = one_hot(iota((lanes, lanes), 0) < iota((lanes, lanes), 1))
        below = one_hot(iota((slots, slots), 1) < iota((slots, slots), 0))
        goal = iota((LANES, lanes), 0).astype(f32).astype(bf16)
        yes, no = jnp.ones((LANES, lanes), bf16), jnp.zeros((LANES, lanes), bf16)
        chunk[...] = jnp.zeros(chunk.shape, f32)
        own[...] = jnp.zeros(own.shape, f32)
        rank_rows = []
        for c in range(2):
            pieces, codes = [], []
            for s in range(slots):
                x = data[s * SLOT_LANES + c * FIELDS : s * SLOT_LANES + (c + 1) * FIELDS, :]
                code = x[5:6, :]
                filled = code > 0.5
                cell = code.astype(i32) - 1
                row = jnp.where(is_own, cell >> 6, jnp.where(is_low, -1, 2)).astype(f32)
                away = jnp.where(is_own, 0, jnp.where(is_low, 512, 256))
                own_row = jnp.where(is_own, (cell >> 6) * ROW_BIT, 0)
                seen = ((cell & (NCOL - 1)) - away + EMPTY_BIT + own_row).astype(f32)
                x = jnp.where(row8 == 1, x + row, jnp.where(row8 == 5, seen, x))
                pieces.append(jnp.where(filled, x, 0.0))
                codes.append(code)
            filled = jnp.concatenate(codes, axis=0) > 0.5
            lane_s = iota((slots, lanes), 1)
            flag_own = jnp.where(filled & (lane_s < peers), 1.0, 0.0)
            flag_far = jnp.where(filled & (lane_s >= peers), 1.0, 0.0)

            def places(flag):
                inside = dot(flag.astype(bf16), before, ((1,), (0,)))
                totals = jnp.broadcast_to(jnp.sum(flag, axis=1, keepdims=True), (slots, LANES))
                ahead = dot(below, totals.astype(bf16), ((1,), (0,)))
                return inside + ahead[:, 0:1], jnp.sum(totals, axis=0, keepdims=True)

            place_own, count_own = places(flag_own)
            place_far, count_far = places(flag_far)
            place = jnp.where(flag_own > 0.5, place_own, place_far + count_own[:, 0:1])
            place = jnp.where(filled, place, -1.0)
            count = count_own + count_far
            rank_rows.append(place[:, 0:LANES])
            stacked = [jnp.concatenate(split3(p), axis=0) for p in pieces]
            total = jnp.max(count)
            for t in range(tiles):

                @pl.when(total > t * LANES)
                def _(t=t, c=c, place=place, stacked=stacked, count_own=count_own):
                    near_place = (place - float(t * LANES)).astype(bf16)
                    acc = jnp.zeros((3 * FIELDS, LANES), f32)
                    for s in range(slots):
                        pick = jnp.where(goal == near_place[s : s + 1, :], yes, no)
                        acc = acc + dot(stacked[s], pick, ((1,), (1,)))
                    x = acc[0:8, :] + acc[8:16, :] + acc[16:24, :]
                    at = t * 2 * USED + c * USED
                    chunk[at : at + USED, :] = x[0:USED, :]
                    if t * LANES < own.shape[1]:
                        x = jnp.where(row_of == 7, count_own, x)
                        own[c * FIELDS : (c + 1) * FIELDS, t * LANES : (t + 1) * LANES] = x

        ranks[...] = jnp.transpose(jnp.concatenate(rank_rows + [jnp.zeros((LANES - 2 * slots, LANES), f32)], axis=0))
        value = chunk[...]
        for d in range(members):
            out[d] = value

    return body


def prepare_body(peers, slots):
    used = 2 * USED

    def body(own, ranks, wide, pick):
        own_width = peers * slots
        stacked = jnp.concatenate([p.astype(f32) for p in split3(own[...])], axis=0)
        columns = jnp.transpose(stacked).astype(bf16)
        spread_to = iota((6 * FIELDS, used * LANES), 1) >> 7
        field_of = spread_to + jnp.where(spread_to >= USED, FIELDS - USED, 0)
        spread = one_hot((iota((6 * FIELDS, used * LANES), 0) & (2 * FIELDS - 1)) == field_of)
        wide[...] = dot(columns, spread, ((1,), (0,)))
        goal = iota((peers, own_width), 1).astype(f32)
        for c in range(2):
            for s in range(slots):
                rank = ranks[0:peers, c * slots + s : c * slots + s + 1]
                pick[s * peers : (s + 1) * peers, c * own_width : (c + 1) * own_width] = one_hot(rank == goal)

    return body


def match_body(peers, slots, members, width):
    block = 8 * GROUPS
    tiles = width // LANES
    rows = message_rows(width)
    usual = tiles * 5 // 12
    own_width = peers * slots
    early = own_width * 5 // 8

    def body(near, own, wide, pick, out, line, totals, values):
        lane8 = iota((8, LANES), 1)
        count_own = [jnp.max(own[c * FIELDS + 7 : c * FIELDS + 8, 0:LANES]).astype(i32) for c in range(2)]

        def count_of(d, c):
            codes = near[pl.ds(d * rows + c * USED + USED - 1, tiles, stride=2 * USED), :]
            return jnp.sum(jnp.where(codes > 0.5, 1.0, 0.0)).astype(i32)

        counts = [[count_of(d, c) for d in range(members)] for c in range(2)]
        ends = []
        for c in range(2):
            start = jnp.int32(0)
            for d in range(members):
                shift = start & (LANES - 1)
                base = start >> 7
                keep = lane8 >= shift

                def put(k, x, c=c, base=base):
                    line[c, base + k] = x

                def turned(k, c=c, d=d, shift=shift):
                    at = d * rows + k * 2 * USED + c * USED
                    return pltpu.roll(near[at : at + FIELDS, :], shift, 1)

                last = jnp.zeros((FIELDS, LANES), f32) if d == 0 else line[c, base]
                for k in range(usual):
                    now = turned(k)
                    put(k, jnp.where(keep, now, last))
                    last = now
                put(usual, jnp.where(keep, 0.0, last))
                put(usual + 1, jnp.zeros((FIELDS, LANES), f32))

                @pl.when(counts[c][d] > usual * LANES)
                def _(c=c, base=base, keep=keep, put=put, turned=turned):
                    last = line[c, base + usual]
                    for k in range(usual, tiles):
                        now = turned(k)
                        put(k, jnp.where(keep, now, last))
                        last = now
                    put(tiles, jnp.where(keep, 0.0, last))
                    put(tiles + 1, jnp.zeros((FIELDS, LANES), f32))

                start = start + counts[c][d]
            ends.append(lax.div(start + (2 * LANES - 1), 2 * LANES))

        for c in range(2):
            other = 1 - c
            blocks = lax.div(count_own[c] + (block - 1), block)

            def own_block(b, _, c=c, other=other):
                base = pl.multiple_of(b * block, 8)
                fields = []
                for g in range(GROUPS):
                    col = [wide[pl.ds(base + 8 * g, 8), (c * USED + f) * LANES : (c * USED + f + 1) * LANES] for f in range(USED)]
                    code = col[5].astype(i32)
                    own_code = code + (NCOL + 1 - EMPTY_BIT)
                    mask = jnp.where(code < ROW_BIT, 256, 512) | (EMPTY_BIT | (NCOL - 1))
                    fields.append((col[0] - 1.0, col[1], col[2], col[3], col[4], own_code, mask))

                def pairs(t, acc):
                    acc = [list(a) for a in acc]
                    for half in range(2):
                        at = line.at[other, 2 * t + half]
                        row = [jnp.broadcast_to(at[f : f + 1, :], (8, LANES)) for f in range(USED)]
                        code = row[5].astype(i32) - EMPTY_BIT
                        for g in range(GROUPS):
                            px, py, xx, yy, xy, own_code, mask = fields[g]
                            step = (own_code - code) & mask
                            dx = step.astype(f32) + (px - row[0])
                            dy = py - row[1]
                            sx, sy, sxy = xx + row[2], yy + row[3], xy + row[4]
                            det = sx * sy - 0.25 * (sxy * sxy)
                            root = lax.rsqrt(det)
                            chi = dy * (sxy * dx - sx * dy) - sy * (dx * dx)
                            like = jnp.exp2(chi * (root * root)) * root
                            like = jnp.where(step <= 2, like, 0.0)
                            acc[g][0] = acc[g][0] + like
                            if c == 0:
                                acc[g][1] = acc[g][1] + like * dx
                                acc[g][2] = acc[g][2] + like * dy
                    return tuple(tuple(a) for a in acc)

                zero = jnp.zeros((8, LANES), f32)
                acc = tuple((zero,) * (3 if c == 0 else 1) for _ in range(GROUPS))
                acc = lax.fori_loop(0, ends[other], pairs, acc)
                for g in range(GROUPS):
                    for k, a in enumerate(acc[g]):
                        totals[3 * c + k, pl.ds(base + 8 * g, 8), :] = a
                return 0

            lax.fori_loop(0, blocks, own_block, 0)

        f_of_lane = lane8 & (SLOT_LANES - 1)

        def sum_rows(first, last):
            for c in range(2):
                for g in range(first // 8, last // 8):
                    live = (iota((8, LANES), 0) + 8 * g) < count_own[c]
                    value = jnp.zeros((8, LANES), f32)
                    for k in range(3 if c == 0 else 1):
                        total = jnp.sum(totals[3 * c + k, 8 * g : 8 * g + 8, :], axis=1, keepdims=True) * GAIN
                        value = jnp.where(f_of_lane == c * FIELDS + k, total, value)
                    values[c * own_width + 8 * g : c * own_width + 8 * g + 8, :] = jnp.where(live, value, 0.0)

        many = jnp.maximum(count_own[0], count_own[1]) > early
        sum_rows(0, early)

        @pl.when(many)
        def _():
            sum_rows(early, own_width)

        @pl.when(jnp.logical_not(many))
        def _():
            for c in range(2):
                values[c * own_width + early : (c + 1) * own_width, :] = jnp.zeros((own_width - early, LANES), f32)

        result = sum(dot(pick[...], part, ((1,), (0,))) for part in split3(values[...]))
        slot_of_lane = iota((peers, LANES), 1) >> 4
        final = jnp.zeros((peers, LANES), f32)
        for s in range(slots):
            final = final + jnp.where(slot_of_lane == s, result[s * peers : (s + 1) * peers, :], 0.0)
        out[...] = final

    return body


def return_body(pix_count, sub_count, peers):
    slots = CAP * sub_count
    turn = first_peer(pix_count, peers)

    def body(back, gd, wd, like, offset, wise):
        n = gd.shape[1]
        own_g, own_w, rank_g, rank_w = owners_and_ranks(gd[...], wd[...], sub_count)
        owner = jnp.concatenate([own_g, own_w], axis=1)
        pick = one_hot(iota((peers, 2 * n), 0) == ((owner + turn) & (peers - 1)))
        turned = jnp.transpose(back[...])
        found = sum(dot(part, pick, ((1,), (0,))) for part in split3(turned))
        gaia = jnp.zeros((FIELDS, n), f32)
        other = jnp.zeros((FIELDS, n), f32)
        for s in range(slots):
            at = s * SLOT_LANES
            gaia = gaia + jnp.where(rank_g == s, found[at : at + FIELDS, 0:n], 0.0)
            other = other + jnp.where(rank_w == s, found[at + FIELDS : at + 2 * FIELDS, n : 2 * n], 0.0)
        like[...] = gaia[0:1, :]
        offset[...] = gaia[1:3, :]
        wise[...] = other[0:1, :]

    return body


def stages(pix_count, sub_count, rep_count, n):
    peers = pix_count * rep_count
    slots = CAP * sub_count
    width = 3 * peers * slots
    own_width = peers * slots
    rows = message_rows(width)
    send = call(send_body(pix_count, sub_count, peers), jax.ShapeDtypeStruct((3 * peers, LANES), f32))
    compact = call(
        compact_body(peers, slots, sub_count, width),
        (
            jax.ShapeDtypeStruct((sub_count, rows, LANES), f32),
            jax.ShapeDtypeStruct((2 * FIELDS, own_width), f32),
            jax.ShapeDtypeStruct((LANES, LANES), f32),
        ),
        [pltpu.VMEM((rows, LANES), f32)],
    )
    prepare = call(
        prepare_body(peers, slots),
        (
            jax.ShapeDtypeStruct((own_width, 2 * USED * LANES), f32),
            jax.ShapeDtypeStruct((own_width, 2 * own_width), bf16),
        ),
    )
    match = call(
        match_body(peers, slots, sub_count, width),
        jax.ShapeDtypeStruct((peers, LANES), f32),
        [
            pltpu.VMEM((2, sub_count * width // LANES + 8, FIELDS, LANES), f32),
            pltpu.VMEM((4, own_width, LANES), f32),
            pltpu.VMEM((2 * own_width, LANES), f32),
        ],
    )
    back = call(
        return_body(pix_count, sub_count, peers),
        (
            jax.ShapeDtypeStruct((1, n), f32),
            jax.ShapeDtypeStruct((2, n), f32),
            jax.ShapeDtypeStruct((1, n), f32),
        ),
    )
    return send, compact, prepare, match, back


def shards(gaia_pos, gaia_shape, gaia_corr, gaia_dest, gaia_cell, wise_pos, wise_shape, wise_corr, wise_dest, wise_cell):
    pix_count = lax.axis_size("pix")
    sub_count = lax.axis_size("sub")
    rep_count = lax.axis_size("rep")
    peers = pix_count * rep_count
    n = gaia_pos.shape[1]
    send, compact, prepare, match, back = stages(pix_count, sub_count, rep_count, n)
    row = lambda x: x.reshape(1, n)
    gd, wd = row(gaia_dest), row(wise_dest)
    msg = send(gaia_pos, gaia_shape, row(gaia_corr), gd, row(gaia_cell), wise_pos, wise_shape, row(wise_corr), wd, row(wise_cell))
    got = lax.all_to_all(msg.reshape(peers, 1, 3 * LANES), ("pix", "rep"), 0, 0, tiled=True)
    chunks, own, ranks = compact(got.reshape(3 * peers, LANES))
    near = lax.all_to_all(chunks, "sub", 0, 0, tiled=True)
    wide, pick = prepare(own, ranks)
    results = match(near.reshape(-1, LANES), own, wide, pick)
    returned = lax.all_to_all(results.reshape(peers, 1, LANES), ("pix", "rep"), 0, 0, tiled=True)
    like, offset, wise = back(returned.reshape(peers, LANES), gd, wd)
    return like.reshape(n), offset, wise.reshape(n)


def solution(mesh):
    flat = P(("groups", "pix", "sub", "rep"))
    pair = P(None, ("groups", "pix", "sub", "rep"))
    column = P(("groups", "pix", "sub", "rep"), None)
    return jax.shard_map(
        shards,
        mesh=mesh,
        in_specs=(pair, pair, flat, column, flat, pair, pair, flat, column, flat),
        out_specs=(flat, pair, flat),
        check_vma=False,
    )
```

```python
import math

import jax
import jax.numpy as jnp
from jax import lax
from jax.experimental import pallas as pl
from jax.experimental.pallas import tpu as pltpu
from jax.sharding import PartitionSpec as P

NCOL = 64
CAP = 2
LANES = 128
SLOT_LANES = 16
FIELDS = 8
EMPTY_BIT = 4096
ROW_BIT = 8192
LAMBDA = 2.0 * math.log(2.0)
GAIN = LAMBDA / (2.0 * math.pi)
GROUPS = 6
USED = 6
INTERPRET = False

f32 = jnp.float32
bf16 = jnp.bfloat16
i32 = jnp.int32


def iota(shape, dim):
    return lax.broadcasted_iota(i32, shape, dim)


def split3(x):
    high = x.astype(bf16)
    rest = x - high.astype(f32)
    middle = rest.astype(bf16)
    low = (rest - middle.astype(f32)).astype(bf16)
    return high, middle, low


def dot(a, b, contract):
    return lax.dot_general(a, b, (contract, ((), ())), preferred_element_type=f32)


def one_hot(mask):
    return jnp.where(mask, 1.0, 0.0).astype(bf16)


def call(body, outs, scratch=(), grant=8 << 20, **more):
    return pl.pallas_call(
        body,
        out_shape=outs,
        **more,
        scratch_shapes=list(scratch),
        compiler_params=pltpu.CompilerParams(vmem_limit_bytes=grant),
        interpret=INTERPRET,
    )


def ring_start(pix_count):
    return pix_count * 3 // 4


def message_rows(width):
    return width // LANES * 2 * USED + FIELDS


def owners_and_ranks(dest_g, dest_w, sub_count):
    n = dest_g.shape[1]
    shift = sub_count.bit_length() - 1
    own_g, own_w = dest_g >> shift, dest_w >> shift
    both = jnp.concatenate([own_g.astype(f32), own_w.astype(f32), jnp.zeros((6, n), f32)], axis=0)
    columns = jnp.transpose(both)
    earlier = iota((n, n), 0) < iota((n, n), 1)

    def rank(row, column):
        same = (row.astype(f32) == column) & earlier
        return jnp.sum(jnp.where(same, 1.0, 0.0), axis=0, keepdims=True).astype(i32)

    return own_g, own_w, rank(own_g, columns[:, 0:1]), rank(own_w, columns[:, 1:2])


def send_body(pix_count, sub_count, peers):
    slots = CAP * sub_count
    turn = pix_count - ring_start(pix_count)

    def body(*refs):
        gp, gs, gc, gd, gl, wp, ws, wc, wd, wl, msg, places = refs
        n = gp.shape[1]
        own_g, own_w, rank_g, rank_w = owners_and_ranks(gd[...], wd[...], sub_count)

        def fields(pos, shape, corr, cell):
            a, b = shape[0:1, :], shape[1:2, :]
            return jnp.concatenate(
                [
                    pos[0:1, :],
                    pos[1:2, :],
                    (a * a) * LAMBDA,
                    (b * b) * LAMBDA,
                    ((corr * a) * b) * (2.0 * LAMBDA),
                    cell.astype(f32) + 1.0,
                    jnp.zeros((2, n), f32),
                ],
                axis=0,
            )

        data_g = fields(gp, gs, gc[...], gl[...])
        data_w = fields(wp, ws, wc[...], wl[...])
        zero = jnp.zeros((FIELDS, n), f32)
        left, right = [], []
        for s in range(slots):
            left += [jnp.where(rank_g == s, data_g, 0.0), zero]
            right += [zero, jnp.where(rank_w == s, data_w, 0.0)]
        table = jnp.concatenate([jnp.concatenate(left, axis=0), jnp.concatenate(right, axis=0)], axis=1)
        rows = 3 * peers
        r = iota((rows, 2 * n), 0)
        peer = jnp.floor((r.astype(f32) + 0.5) * (1.0 / 3.0)).astype(i32)
        side = r - 3 * peer
        band = (peer - turn) & (peers - 1)
        owner = jnp.concatenate([own_g, own_w], axis=1)
        upper = jnp.concatenate([gl[...], wl[...]], axis=1) >> (NCOL.bit_length() - 1)
        edge = (side == 1) | (upper == jnp.where(side == 0, 1, 0))
        pick = one_hot((owner == band + side - 1) & (band < pix_count) & edge)
        msg[...] = sum(dot(pick, part, ((1,), (1,))) for part in split3(table))
        at = [(o + turn) & (peers - 1) for o in (own_g, own_w)]
        places[...] = jnp.concatenate(at + [rank_g, rank_w, jnp.zeros((4, n), i32)], axis=0)

    return body


def compact_body(peers, slots, members, width):
    lanes = -(-3 * peers // LANES) * LANES
    tiles = width // LANES

    def body(got, out, own, ranks, chunk):
        parts = [got[pl.ds(j, peers, stride=3), :] for j in (1, 0, 2)]
        parts.append(jnp.zeros((lanes - 3 * peers, LANES), f32))
        data = jnp.transpose(jnp.concatenate(parts, axis=0))
        lane8 = iota((FIELDS, lanes), 1)
        row8 = iota((FIELDS, lanes), 0)
        row_of = iota((FIELDS, LANES), 0)
        is_own = lane8 < peers
        is_low = (lane8 >= peers) & (lane8 < 2 * peers)
        before = one_hot(iota((lanes, lanes), 0) < iota((lanes, lanes), 1))
        below = one_hot(iota((slots, slots), 1) < iota((slots, slots), 0))
        goal = iota((LANES, lanes), 0).astype(f32).astype(bf16)
        yes, no = jnp.ones((LANES, lanes), bf16), jnp.zeros((LANES, lanes), bf16)
        chunk[...] = jnp.zeros(chunk.shape, f32)
        own[...] = jnp.zeros(own.shape, f32)
        rank_rows = []
        for c in range(2):
            pieces, codes = [], []
            for s in range(slots):
                x = data[s * SLOT_LANES + c * FIELDS : s * SLOT_LANES + (c + 1) * FIELDS, :]
                code = x[5:6, :]
                filled = code > 0.5
                cell = code.astype(i32) - 1
                row = jnp.where(is_own, cell >> 6, jnp.where(is_low, -1, 2)).astype(f32)
                away = jnp.where(is_own, 0, jnp.where(is_low, 512, 256))
                own_row = jnp.where(is_own, (cell >> 6) * ROW_BIT, 0)
                seen = ((cell & (NCOL - 1)) - away + EMPTY_BIT + own_row).astype(f32)
                x = jnp.where(row8 == 1, x + row, jnp.where(row8 == 5, seen, x))
                pieces.append(jnp.where(filled, x, 0.0))
                codes.append(code)
            filled = jnp.concatenate(codes, axis=0) > 0.5
            lane_s = iota((slots, lanes), 1)
            flag_own = jnp.where(filled & (lane_s < peers), 1.0, 0.0)
            flag_far = jnp.where(filled & (lane_s >= peers), 1.0, 0.0)

            def places(flag):
                inside = dot(flag.astype(bf16), before, ((1,), (0,)))
                totals = jnp.broadcast_to(jnp.sum(flag, axis=1, keepdims=True), (slots, LANES))
                ahead = dot(below, totals.astype(bf16), ((1,), (0,)))
                return inside + ahead[:, 0:1], jnp.sum(totals, axis=0, keepdims=True)

            place_own, count_own = places(flag_own)
            place_far, count_far = places(flag_far)
            place = jnp.where(flag_own > 0.5, place_own, place_far + count_own[:, 0:1])
            place = jnp.where(filled, place, -1.0)
            count = count_own + count_far
            rank_rows.append(place[:, 0:LANES])
            stacked = [jnp.concatenate(split3(p), axis=0) for p in pieces]
            total = jnp.max(count)
            for t in range(tiles):

                @pl.when(total > t * LANES)
                def _(t=t, c=c, place=place, stacked=stacked, count_own=count_own):
                    near_place = (place - float(t * LANES)).astype(bf16)
                    acc = jnp.zeros((3 * FIELDS, LANES), f32)
                    for s in range(slots):
                        pick = jnp.where(goal == near_place[s : s + 1, :], yes, no)
                        acc = acc + dot(stacked[s], pick, ((1,), (1,)))
                    x = acc[0:8, :] + acc[8:16, :] + acc[16:24, :]
                    at = t * 2 * USED + c * USED
                    chunk[at : at + USED, :] = x[0:USED, :]
                    if t * LANES < own.shape[1]:
                        x = jnp.where(row_of == 7, count_own, x)
                        own[c * FIELDS : (c + 1) * FIELDS, t * LANES : (t + 1) * LANES] = x

        ranks[...] = jnp.transpose(jnp.concatenate(rank_rows + [jnp.zeros((LANES - 2 * slots, LANES), f32)], axis=0))
        value = chunk[...]
        for d in range(members):
            out[d] = value

    return body


def prepare_body(peers, slots):
    used = 2 * USED

    def body(own, ranks, wide, pick):
        own_width = peers * slots
        stacked = jnp.concatenate([p.astype(f32) for p in split3(own[...])], axis=0)
        columns = jnp.transpose(stacked).astype(bf16)
        spread_to = iota((6 * FIELDS, used * LANES), 1) >> 7
        field_of = spread_to + jnp.where(spread_to >= USED, FIELDS - USED, 0)
        spread = one_hot((iota((6 * FIELDS, used * LANES), 0) & (2 * FIELDS - 1)) == field_of)
        wide[0:own_width, :] = dot(columns, spread, ((1,), (0,)))
        wide[own_width:, :] = jnp.zeros((8 * GROUPS, used * LANES), f32)
        goal = iota((peers, own_width), 1).astype(f32)
        for c in range(2):
            for s in range(slots):
                rank = ranks[0:peers, c * slots + s : c * slots + s + 1]
                pick[s * peers : (s + 1) * peers, c * own_width : (c + 1) * own_width] = one_hot(rank == goal)

    return body


def match_body(peers, slots, members, width):
    block = 8 * GROUPS
    tiles = width // LANES
    rows = message_rows(width)
    usual = tiles // 2
    own_width = peers * slots
    early = own_width * 5 // 8

    prepare = prepare_body(peers, slots)

    def body(near, own, ranks, out, wide, pick, line, totals, values):
        prepare(own, ranks, wide, pick)
        lane8 = iota((8, LANES), 1)
        count_own = [jnp.max(own[c * FIELDS + 7 : c * FIELDS + 8, 0:LANES]).astype(i32) for c in range(2)]

        def count_of(d, c):
            codes = near[pl.ds(d * rows + c * USED + USED - 1, tiles, stride=2 * USED), :]
            return jnp.sum(jnp.where(codes > 0.5, 1.0, 0.0)).astype(i32)

        counts = [[count_of(d, c) for d in range(members)] for c in range(2)]
        ends = []
        for c in range(2):
            start = jnp.int32(0)
            for d in range(members):
                shift = start & (LANES - 1)
                base = start >> 7
                keep = lane8 >= shift

                def put(k, x, c=c, base=base):
                    line[c, base + k] = x

                def turned(k, c=c, d=d, shift=shift):
                    at = d * rows + k * 2 * USED + c * USED
                    return pltpu.roll(near[at : at + FIELDS, :], shift, 1)

                last = jnp.zeros((FIELDS, LANES), f32) if d == 0 else line[c, base]
                for k in range(usual):
                    now = turned(k)
                    put(k, jnp.where(keep, now, last))
                    last = now
                put(usual, jnp.where(keep, 0.0, last))
                put(usual + 1, jnp.zeros((FIELDS, LANES), f32))

                @pl.when(counts[c][d] > usual * LANES)
                def _(c=c, base=base, keep=keep, put=put, turned=turned):
                    last = line[c, base + usual]
                    for k in range(usual, tiles):
                        now = turned(k)
                        put(k, jnp.where(keep, now, last))
                        last = now
                    put(tiles, jnp.where(keep, 0.0, last))
                    put(tiles + 1, jnp.zeros((FIELDS, LANES), f32))

                start = start + counts[c][d]
            ends.append(lax.div(start + (2 * LANES - 1), 2 * LANES))

        for c in range(2):
            other = 1 - c
            blocks = lax.div(count_own[c] + (block - 1), block)

            def own_block(b, _, c=c, other=other):
                base = pl.multiple_of(b * block, 8)
                fields = []
                for g in range(GROUPS):
                    col = [wide[pl.ds(base + 8 * g, 8), (c * USED + f) * LANES : (c * USED + f + 1) * LANES] for f in range(USED)]
                    code = col[5].astype(i32)
                    own_code = code + (NCOL + 1 - EMPTY_BIT)
                    mask = jnp.where(code < ROW_BIT, 256, 512) | (EMPTY_BIT | (NCOL - 1))
                    fields.append((col[0] - 1.0, col[1], col[2], col[3], col[4], own_code, mask))

                def pairs(t, acc):
                    acc = [list(a) for a in acc]
                    for half in range(2):
                        at = line.at[other, 2 * t + half]
                        row = [jnp.broadcast_to(at[f : f + 1, :], (8, LANES)) for f in range(USED)]
                        code = row[5].astype(i32) - EMPTY_BIT
                        for g in range(GROUPS):
                            px, py, xx, yy, xy, own_code, mask = fields[g]
                            step = (own_code - code) & mask
                            dx = step.astype(f32) + (px - row[0])
                            dy = py - row[1]
                            sx, sy, sxy = xx + row[2], yy + row[3], xy + row[4]
                            det = sx * sy - 0.25 * (sxy * sxy)
                            root = lax.rsqrt(det)
                            chi = dy * (sxy * dx - sx * dy) - sy * (dx * dx)
                            like = jnp.exp2(chi * (root * root)) * root
                            like = jnp.where(step <= 2, like, 0.0)
                            acc[g][0] = acc[g][0] + like
                            if c == 0:
                                acc[g][1] = acc[g][1] + like * dx
                                acc[g][2] = acc[g][2] + like * dy
                    return tuple(tuple(a) for a in acc)

                zero = jnp.zeros((8, LANES), f32)
                acc = tuple((zero,) * (3 if c == 0 else 1) for _ in range(GROUPS))
                acc = lax.fori_loop(0, ends[other], pairs, acc)
                for g in range(GROUPS):
                    for k, a in enumerate(acc[g]):
                        totals[3 * c + k, pl.ds(base + 8 * g, 8), :] = a
                return 0

            lax.fori_loop(0, blocks, own_block, 0)

        f_of_lane = lane8 & (SLOT_LANES - 1)

        def sum_rows(first, last):
            for c in range(2):
                for g in range(first // 8, last // 8):
                    live = (iota((8, LANES), 0) + 8 * g) < count_own[c]
                    value = jnp.zeros((8, LANES), f32)
                    for k in range(3 if c == 0 else 1):
                        total = jnp.sum(totals[3 * c + k, 8 * g : 8 * g + 8, :], axis=1, keepdims=True) * GAIN
                        value = jnp.where(f_of_lane == c * FIELDS + k, total, value)
                    values[c * own_width + 8 * g : c * own_width + 8 * g + 8, :] = jnp.where(live, value, 0.0)

        many = jnp.maximum(count_own[0], count_own[1]) > early
        sum_rows(0, early)

        @pl.when(many)
        def _():
            sum_rows(early, own_width)

        @pl.when(jnp.logical_not(many))
        def _():
            for c in range(2):
                values[c * own_width + early : (c + 1) * own_width, :] = jnp.zeros((own_width - early, LANES), f32)

        result = sum(dot(pick[...], part, ((1,), (0,))) for part in split3(values[...]))
        slot_of_lane = iota((peers, LANES), 1) >> 4
        final = jnp.zeros((peers, LANES), f32)
        for s in range(slots):
            final = final + jnp.where(slot_of_lane == s, result[s * peers : (s + 1) * peers, :], 0.0)
        out[...] = final

    return body


def return_body(sub_count, peers):
    slots = CAP * sub_count

    def body(back, places, like, offset, wise):
        n = places.shape[1]
        at = jnp.concatenate([places[0:1, :], places[1:2, :]], axis=1)
        rank_g, rank_w = places[2:3, :], places[3:4, :]
        pick = one_hot(iota((peers, 2 * n), 0) == at)
        turned = jnp.transpose(back[...])
        found = sum(dot(part, pick, ((1,), (0,))) for part in split3(turned))
        gaia = jnp.zeros((FIELDS, n), f32)
        other = jnp.zeros((FIELDS, n), f32)
        for s in range(slots):
            at = s * SLOT_LANES
            gaia = gaia + jnp.where(rank_g == s, found[at : at + FIELDS, 0:n], 0.0)
            other = other + jnp.where(rank_w == s, found[at + FIELDS : at + 2 * FIELDS, n : 2 * n], 0.0)
        like[...] = gaia[0:1, :]
        offset[...] = gaia[1:3, :]
        wise[...] = other[0:1, :]

    return body


def stages(pix_count, sub_count, rep_count, n):
    peers = pix_count
    members = sub_count * rep_count
    slots = CAP * sub_count
    width = 3 * peers * slots
    own_width = peers * slots
    rows = message_rows(width)
    pair, line, whole = pltpu.VMEM((2, n), f32), pltpu.VMEM((1, n), f32), pltpu.VMEM((1, n), i32)
    send = call(
        send_body(pix_count, sub_count, peers),
        (jax.ShapeDtypeStruct((3 * peers, LANES), f32), jax.ShapeDtypeStruct((8, n), i32)),
    )
    compact = call(
        compact_body(peers, slots, members, width),
        (
            jax.ShapeDtypeStruct((members, rows, LANES), f32),
            jax.ShapeDtypeStruct((2 * FIELDS, own_width), f32),
            jax.ShapeDtypeStruct((LANES, LANES), f32),
        ),
        [pltpu.VMEM((rows, LANES), f32)],
    )
    match = call(
        match_body(peers, slots, members, width),
        jax.ShapeDtypeStruct((peers, LANES), f32),
        [
            pltpu.VMEM((own_width + 8 * GROUPS, 2 * USED * LANES), f32),
            pltpu.VMEM((own_width, 2 * own_width), bf16),
            pltpu.VMEM((2, members * width // LANES + 8, FIELDS, LANES), f32),
            pltpu.VMEM((4, own_width + 8 * GROUPS, LANES), f32),
            pltpu.VMEM((2 * own_width, LANES), f32),
        ],
    )
    back = call(
        return_body(sub_count, peers),
        (
            jax.ShapeDtypeStruct((1, n), f32),
            jax.ShapeDtypeStruct((2, n), f32),
            jax.ShapeDtypeStruct((1, n), f32),
        ),
    )
    return send, compact, match, back


def shards(gaia_pos, gaia_shape, gaia_corr, gaia_dest, gaia_cell, wise_pos, wise_shape, wise_corr, wise_dest, wise_cell):
    pix_count = lax.axis_size("pix")
    sub_count = lax.axis_size("sub")
    rep_count = lax.axis_size("rep")
    peers = pix_count
    n = gaia_pos.shape[1]
    send, compact, match, back = stages(pix_count, sub_count, rep_count, n)
    row = lambda x: x.reshape(1, n)
    gd, wd = row(gaia_dest), row(wise_dest)
    msg, places = send(gaia_pos, gaia_shape, row(gaia_corr), gd, row(gaia_cell), wise_pos, wise_shape, row(wise_corr), wd, row(wise_cell))
    ring = [[(i + ring_start(pix_count)) % pix_count for i in range(pix_count)]]
    exchange = lambda x: lax.all_to_all(x, "pix", 0, 0, axis_index_groups=ring, tiled=True)
    got = exchange(msg.reshape(peers, 1, 3 * LANES))
    chunks, own, ranks = compact(got.reshape(3 * peers, LANES))
    near = lax.all_to_all(chunks, ("sub", "rep"), 0, 0, tiled=True)
    results = match(near.reshape(-1, LANES), own, ranks)
    returned = exchange(results.reshape(peers, 1, LANES))
    like, offset, wise = back(returned.reshape(peers, LANES), places)
    return like.reshape(n), offset, wise.reshape(n)


def solution(mesh):
    flat = P(("groups", "pix", "sub", "rep"))
    pair = P(None, ("groups", "pix", "sub", "rep"))
    column = P(("groups", "pix", "sub", "rep"), None)
    return jax.shard_map(
        shards,
        mesh=mesh,
        in_specs=(pair, pair, flat, column, flat, pair, pair, flat, column, flat),
        out_specs=(flat, pair, flat),
        check_vma=False,
    )
```

```python
import math

import jax
import jax.numpy as jnp
from jax import lax
from jax.experimental import pallas as pl
from jax.experimental.pallas import tpu as pltpu
from jax.sharding import PartitionSpec as P

NCOL = 64
CAP = 2
LANES = 128
SLOT_LANES = 16
FIELDS = 8
EMPTY_BIT = 4096
ROW_BIT = 8192
LAMBDA = 2.0 * math.log(2.0)
GAIN = LAMBDA / (2.0 * math.pi)
GROUPS = 6
USED = 6
PART = 3
INTERPRET = False

f32 = jnp.float32
bf16 = jnp.bfloat16
i32 = jnp.int32


def iota(shape, dim):
    return lax.broadcasted_iota(i32, shape, dim)


def split3(x):
    high = x.astype(bf16)
    rest = x - high.astype(f32)
    middle = rest.astype(bf16)
    low = (rest - middle.astype(f32)).astype(bf16)
    return high, middle, low


def dot(a, b, contract):
    return lax.dot_general(a, b, (contract, ((), ())), preferred_element_type=f32)


def one_hot(mask):
    return jnp.where(mask, 1.0, 0.0).astype(bf16)


def call(body, outs, scratch=(), grant=8 << 20, **more):
    return pl.pallas_call(
        body,
        out_shape=outs,
        **more,
        scratch_shapes=list(scratch),
        compiler_params=pltpu.CompilerParams(vmem_limit_bytes=grant),
        interpret=INTERPRET,
    )


def ring_start(pix_count):
    return pix_count * 3 // 4


def part_rows():
    return -(-(PART * 2 * USED + 2) // 8) * 8


def tile_row(t, c):
    return t // PART * part_rows() + t % PART * 2 * USED + c * USED


def owners_and_ranks(dest_g, dest_w, sub_count):
    n = dest_g.shape[1]
    shift = sub_count.bit_length() - 1
    own_g, own_w = dest_g >> shift, dest_w >> shift
    both = jnp.concatenate([own_g.astype(f32), own_w.astype(f32), jnp.zeros((6, n), f32)], axis=0)
    columns = jnp.transpose(both)
    earlier = iota((n, n), 0) < iota((n, n), 1)

    def rank(row, column):
        same = (row.astype(f32) == column) & earlier
        return jnp.sum(jnp.where(same, 1.0, 0.0), axis=0, keepdims=True).astype(i32)

    return own_g, own_w, rank(own_g, columns[:, 0:1]), rank(own_w, columns[:, 1:2])


def send_body(pix_count, sub_count, peers):
    slots = CAP * sub_count
    turn = pix_count - ring_start(pix_count)

    def body(*refs):
        gp, gs, gc, gd, gl, wp, ws, wc, wd, wl, msg, places = refs
        n = gp.shape[1]
        own_g, own_w, rank_g, rank_w = owners_and_ranks(gd[...], wd[...], sub_count)

        def fields(pos, shape, corr, cell):
            a, b = shape[0:1, :], shape[1:2, :]
            return jnp.concatenate(
                [
                    pos[0:1, :],
                    pos[1:2, :],
                    (a * a) * LAMBDA,
                    (b * b) * LAMBDA,
                    ((corr * a) * b) * (2.0 * LAMBDA),
                    cell.astype(f32) + 1.0,
                    jnp.zeros((2, n), f32),
                ],
                axis=0,
            )

        data_g = fields(gp, gs, gc[...], gl[...])
        data_w = fields(wp, ws, wc[...], wl[...])
        zero = jnp.zeros((FIELDS, n), f32)
        left, right = [], []
        for s in range(slots):
            left += [jnp.where(rank_g == s, data_g, 0.0), zero]
            right += [zero, jnp.where(rank_w == s, data_w, 0.0)]
        table = jnp.concatenate([jnp.concatenate(left, axis=0), jnp.concatenate(right, axis=0)], axis=1)
        rows = 3 * peers
        r = iota((rows, 2 * n), 0)
        peer = jnp.floor((r.astype(f32) + 0.5) * (1.0 / 3.0)).astype(i32)
        side = r - 3 * peer
        band = (peer - turn) & (peers - 1)
        owner = jnp.concatenate([own_g, own_w], axis=1)
        upper = jnp.concatenate([gl[...], wl[...]], axis=1) >> (NCOL.bit_length() - 1)
        edge = (side == 1) | (upper == jnp.where(side == 0, 1, 0))
        pick = one_hot((owner == band + side - 1) & (band < pix_count) & edge)
        msg[...] = sum(dot(pick, part, ((1,), (1,))) for part in split3(table))
        at = [(o + turn) & (peers - 1) for o in (own_g, own_w)]
        places[...] = jnp.concatenate(at + [rank_g, rank_w, jnp.zeros((4, n), i32)], axis=0)

    return body


def compact_body(peers, slots, members, width):
    lanes = -(-3 * peers // LANES) * LANES
    tiles = width // LANES

    def body(got, out, rest, own, ranks, chunk):
        parts = [got[pl.ds(j, peers, stride=3), :] for j in (1, 0, 2)]
        parts.append(jnp.zeros((lanes - 3 * peers, LANES), f32))
        data = jnp.transpose(jnp.concatenate(parts, axis=0))
        lane8 = iota((FIELDS, lanes), 1)
        row8 = iota((FIELDS, lanes), 0)
        row_of = iota((FIELDS, LANES), 0)
        is_own = lane8 < peers
        is_low = (lane8 >= peers) & (lane8 < 2 * peers)
        before = one_hot(iota((lanes, lanes), 0) < iota((lanes, lanes), 1))
        below = one_hot(iota((slots, slots), 1) < iota((slots, slots), 0))
        goal = iota((LANES, lanes), 0).astype(f32)
        chunk[...] = jnp.zeros(chunk.shape, f32)
        own[...] = jnp.zeros(own.shape, f32)
        rank_rows = []
        for c in range(2):
            pieces, codes = [], []
            for s in range(slots):
                x = data[s * SLOT_LANES + c * FIELDS : s * SLOT_LANES + (c + 1) * FIELDS, :]
                code = x[5:6, :]
                filled = code > 0.5
                cell = code.astype(i32) - 1
                row = jnp.where(is_own, cell >> 6, jnp.where(is_low, -1, 2)).astype(f32)
                away = jnp.where(is_own, 0, jnp.where(is_low, 512, 256))
                own_row = jnp.where(is_own, (cell >> 6) * ROW_BIT, 0)
                seen = ((cell & (NCOL - 1)) - away + EMPTY_BIT + own_row).astype(f32)
                x = jnp.where(row8 == 1, x + row, jnp.where(row8 == 5, seen, x))
                pieces.append(jnp.where(filled, x, 0.0))
                codes.append(code)
            filled = jnp.concatenate(codes, axis=0) > 0.5
            lane_s = iota((slots, lanes), 1)
            flag_own = jnp.where(filled & (lane_s < peers), 1.0, 0.0)
            flag_far = jnp.where(filled & (lane_s >= peers), 1.0, 0.0)

            def places(flag):
                inside = dot(flag.astype(bf16), before, ((1,), (0,)))
                totals = jnp.broadcast_to(jnp.sum(flag, axis=1, keepdims=True), (slots, LANES))
                ahead = dot(below, totals.astype(bf16), ((1,), (0,)))
                return inside + ahead[:, 0:1], jnp.sum(totals, axis=0, keepdims=True)

            place_own, count_own = places(flag_own)
            place_far, count_far = places(flag_far)
            place = jnp.where(flag_own > 0.5, place_own, place_far + count_own[:, 0:1])
            place = jnp.where(filled, place, -1.0)
            count = count_own + count_far
            rank_rows.append(place[:, 0:LANES])
            stacked = [jnp.concatenate(split3(p), axis=0) for p in pieces]
            total = jnp.max(count)
            chunk[PART * 2 * USED + c : PART * 2 * USED + c + 1, :] = count
            for t in range(tiles):

                @pl.when(total > t * LANES)
                def _(t=t, c=c, place=place, stacked=stacked, count_own=count_own):
                    goal_t = goal + float(t * LANES)
                    acc = jnp.zeros((3 * FIELDS, LANES), f32)
                    for s in range(slots):
                        pick = one_hot(goal_t == place[s : s + 1, :])
                        acc = acc + dot(stacked[s], pick, ((1,), (1,)))
                    x = acc[0:8, :] + acc[8:16, :] + acc[16:24, :]
                    at = tile_row(t, c)
                    chunk[at : at + USED, :] = x[0:USED, :]
                    if t * LANES < own.shape[1]:
                        x = jnp.where(row_of == 7, count_own, x)
                        own[c * FIELDS : (c + 1) * FIELDS, t * LANES : (t + 1) * LANES] = x

        ranks[...] = jnp.transpose(jnp.concatenate(rank_rows + [jnp.zeros((LANES - 2 * slots, LANES), f32)], axis=0))
        value = chunk[0 : part_rows(), :]
        for d in range(members):
            out[d] = value
        rest[...] = chunk[part_rows() :, :]

    return body


def prepare_body(peers, slots):
    used = 2 * USED

    def body(own, ranks, wide, pick):
        own_width = peers * slots
        stacked = jnp.concatenate([p.astype(f32) for p in split3(own[...])], axis=0)
        columns = jnp.transpose(stacked).astype(bf16)
        spread_to = iota((6 * FIELDS, used * LANES), 1) >> 7
        field_of = spread_to + jnp.where(spread_to >= USED, FIELDS - USED, 0)
        spread = one_hot((iota((6 * FIELDS, used * LANES), 0) & (2 * FIELDS - 1)) == field_of)
        wide[0:own_width, :] = dot(columns, spread, ((1,), (0,)))
        wide[own_width:, :] = jnp.zeros((8 * GROUPS, used * LANES), f32)
        goal = iota((peers, own_width), 1).astype(f32)
        for c in range(2):
            for s in range(slots):
                rank = ranks[0:peers, c * slots + s : c * slots + s + 1]
                pick[s * peers : (s + 1) * peers, c * own_width : (c + 1) * own_width] = one_hot(rank == goal)

    return body


def match_body(peers, slots, members, tiles):
    block = 8 * GROUPS
    whole = tiles > PART
    usual = PART
    rows = part_rows()
    own_width = peers * slots
    early = own_width * 5 // 8

    prepare = prepare_body(peers, slots)

    def body(*refs):
        near, refs = refs[: 1 + whole], refs[1 + whole :]
        own, ranks, out, refs = refs[0], refs[1], refs[2], refs[3:]
        over, refs = refs[: 1 - whole], refs[1 - whole :]
        wide, pick, line, totals, values = refs
        prepare(own, ranks, wide, pick)
        lane8 = iota((8, LANES), 1)
        count_own = [jnp.max(own[c * FIELDS + 7 : c * FIELDS + 8, 0:LANES]).astype(i32) for c in range(2)]

        def count_of(d, c):
            at = d * rows + PART * 2 * USED + c
            return jnp.max(near[0][at : at + 1, :]).astype(i32)

        counts = [[count_of(d, c) for d in range(members)] for c in range(2)]
        if not whole:
            most = counts[0][0]
            for n in counts[0][1:] + counts[1]:
                most = jnp.maximum(most, n)
            over[0][0, 0] = (most > PART * LANES).astype(i32)
            counts = [[jnp.minimum(n, PART * LANES) for n in line_counts] for line_counts in counts]
        ends = []
        for c in range(2):
            start = jnp.int32(0)
            for d in range(members):
                shift = start & (LANES - 1)
                base = start >> 7
                keep = lane8 >= shift

                def put(k, x, c=c, base=base):
                    line[c, base + k] = x

                def turned(k, c=c, d=d, shift=shift):
                    at = d * rows + tile_row(k % PART, c)
                    return pltpu.roll(near[k // PART][at : at + FIELDS, :], shift, 1)

                last = jnp.zeros((FIELDS, LANES), f32) if d == 0 else line[c, base]
                for k in range(usual):
                    now = turned(k)
                    put(k, jnp.where(keep, now, last))
                    last = now
                put(usual, jnp.where(keep, 0.0, last))
                put(usual + 1, jnp.zeros((FIELDS, LANES), f32))

                if not whole:
                    start = start + counts[c][d]
                    continue

                @pl.when(counts[c][d] > usual * LANES)
                def _(c=c, base=base, keep=keep, put=put, turned=turned):
                    last = line[c, base + usual]
                    for k in range(usual, tiles):
                        now = turned(k)
                        put(k, jnp.where(keep, now, last))
                        last = now
                    put(tiles, jnp.where(keep, 0.0, last))
                    put(tiles + 1, jnp.zeros((FIELDS, LANES), f32))

                start = start + counts[c][d]
            ends.append(lax.div(start + (2 * LANES - 1), 2 * LANES))

        for c in range(2):
            other = 1 - c
            blocks = lax.div(count_own[c] + (block - 1), block)

            def own_block(b, _, c=c, other=other):
                base = pl.multiple_of(b * block, 8)
                fields = []
                for g in range(GROUPS):
                    col = [wide[pl.ds(base + 8 * g, 8), (c * USED + f) * LANES : (c * USED + f + 1) * LANES] for f in range(USED)]
                    code = col[5].astype(i32)
                    own_code = code + (NCOL + 1 - EMPTY_BIT)
                    mask = jnp.where(code < ROW_BIT, 256, 512) | (EMPTY_BIT | (NCOL - 1))
                    fields.append((col[0] - 1.0, col[1], col[2], col[3], col[4], own_code, mask))

                def pairs(t, acc):
                    acc = [list(a) for a in acc]
                    for half in range(2):
                        at = line.at[other, 2 * t + half]
                        row = [jnp.broadcast_to(at[f : f + 1, :], (8, LANES)) for f in range(USED)]
                        code = row[5].astype(i32) - EMPTY_BIT
                        for g in range(GROUPS):
                            px, py, xx, yy, xy, own_code, mask = fields[g]
                            step = (own_code - code) & mask
                            dx = step.astype(f32) + (px - row[0])
                            dy = py - row[1]
                            sx, sy, sxy = xx + row[2], yy + row[3], xy + row[4]
                            det = sx * sy - 0.25 * (sxy * sxy)
                            root = lax.rsqrt(det)
                            chi = dy * (sxy * dx - sx * dy) - sy * (dx * dx)
                            like = jnp.exp2(chi * (root * root)) * root
                            like = jnp.where(step <= 2, like, 0.0)
                            acc[g][0] = acc[g][0] + like
                            if c == 0:
                                acc[g][1] = acc[g][1] + like * dx
                                acc[g][2] = acc[g][2] + like * dy
                    return tuple(tuple(a) for a in acc)

                zero = jnp.zeros((8, LANES), f32)
                acc = tuple((zero,) * (3 if c == 0 else 1) for _ in range(GROUPS))
                acc = lax.fori_loop(0, ends[other], pairs, acc)
                for g in range(GROUPS):
                    for k, a in enumerate(acc[g]):
                        totals[3 * c + k, pl.ds(base + 8 * g, 8), :] = a
                return 0

            lax.fori_loop(0, blocks, own_block, 0)

        f_of_lane = lane8 & (SLOT_LANES - 1)

        def sum_rows(first, last):
            for c in range(2):
                for g in range(first // 8, last // 8):
                    live = (iota((8, LANES), 0) + 8 * g) < count_own[c]
                    value = jnp.zeros((8, LANES), f32)
                    for k in range(3 if c == 0 else 1):
                        total = jnp.sum(totals[3 * c + k, 8 * g : 8 * g + 8, :], axis=1, keepdims=True) * GAIN
                        value = jnp.where(f_of_lane == c * FIELDS + k, total, value)
                    values[c * own_width + 8 * g : c * own_width + 8 * g + 8, :] = jnp.where(live, value, 0.0)

        many = jnp.maximum(count_own[0], count_own[1]) > early
        sum_rows(0, early)

        @pl.when(many)
        def _():
            sum_rows(early, own_width)

        @pl.when(jnp.logical_not(many))
        def _():
            for c in range(2):
                values[c * own_width + early : (c + 1) * own_width, :] = jnp.zeros((own_width - early, LANES), f32)

        result = sum(dot(pick[...], part, ((1,), (0,))) for part in split3(values[...]))
        slot_of_lane = iota((peers, LANES), 1) >> 4
        final = jnp.zeros((peers, LANES), f32)
        for s in range(slots):
            final = final + jnp.where(slot_of_lane == s, result[s * peers : (s + 1) * peers, :], 0.0)
        out[...] = final

    return body


def return_body(sub_count, peers):
    slots = CAP * sub_count

    def body(back, places, like, offset, wise):
        n = places.shape[1]
        at = jnp.concatenate([places[0:1, :], places[1:2, :]], axis=1)
        rank_g, rank_w = places[2:3, :], places[3:4, :]
        pick = one_hot(iota((peers, 2 * n), 0) == at)
        turned = jnp.transpose(back[...])
        found = sum(dot(part, pick, ((1,), (0,))) for part in split3(turned))
        gaia = jnp.zeros((FIELDS, n), f32)
        other = jnp.zeros((FIELDS, n), f32)
        for s in range(slots):
            at = s * SLOT_LANES
            gaia = gaia + jnp.where(rank_g == s, found[at : at + FIELDS, 0:n], 0.0)
            other = other + jnp.where(rank_w == s, found[at + FIELDS : at + 2 * FIELDS, n : 2 * n], 0.0)
        like[...] = gaia[0:1, :]
        offset[...] = gaia[1:3, :]
        wise[...] = other[0:1, :]

    return body


def stages(pix_count, sub_count, rep_count, n):
    peers = pix_count
    members = sub_count * rep_count
    slots = CAP * sub_count
    width = 3 * peers * slots
    own_width = peers * slots
    rows = part_rows()
    parts = width // LANES // PART
    pair, line, whole = pltpu.VMEM((2, n), f32), pltpu.VMEM((1, n), f32), pltpu.VMEM((1, n), i32)
    send = call(
        send_body(pix_count, sub_count, peers),
        (jax.ShapeDtypeStruct((3 * peers, LANES), f32), jax.ShapeDtypeStruct((8, n), i32)),
    )
    compact = call(
        compact_body(peers, slots, members, width),
        (
            jax.ShapeDtypeStruct((members, rows, LANES), f32),
            jax.ShapeDtypeStruct(((parts - 1) * rows, LANES), f32),
            jax.ShapeDtypeStruct((2 * FIELDS, own_width), f32),
            jax.ShapeDtypeStruct((LANES, LANES), f32),
        ),
        [pltpu.VMEM((parts * rows, LANES), f32)],
    )
    results = jax.ShapeDtypeStruct((peers, LANES), f32)
    held = lambda tiles: [
        pltpu.VMEM((own_width + 8 * GROUPS, 2 * USED * LANES), f32),
        pltpu.VMEM((own_width, 2 * own_width), bf16),
        pltpu.VMEM((2, members * tiles + 8, FIELDS, LANES), f32),
        pltpu.VMEM((4, own_width + 8 * GROUPS, LANES), f32),
        pltpu.VMEM((2 * own_width, LANES), f32),
    ]
    match = call(
        match_body(peers, slots, members, PART),
        (results, jax.ShapeDtypeStruct((1, 1), i32)),
        held(PART),
        out_specs=(pl.BlockSpec(memory_space=pltpu.VMEM), pl.BlockSpec(memory_space=pltpu.SMEM)),
    )
    match_whole = call(match_body(peers, slots, members, width // LANES), results, held(width // LANES))
    back = call(
        return_body(sub_count, peers),
        (
            jax.ShapeDtypeStruct((1, n), f32),
            jax.ShapeDtypeStruct((2, n), f32),
            jax.ShapeDtypeStruct((1, n), f32),
        ),
    )
    return send, compact, match, match_whole, back


def shards(gaia_pos, gaia_shape, gaia_corr, gaia_dest, gaia_cell, wise_pos, wise_shape, wise_corr, wise_dest, wise_cell):
    pix_count = lax.axis_size("pix")
    sub_count = lax.axis_size("sub")
    rep_count = lax.axis_size("rep")
    peers = pix_count
    members = sub_count * rep_count
    n = gaia_pos.shape[1]
    send, compact, match, match_whole, back = stages(pix_count, sub_count, rep_count, n)
    row = lambda x: x.reshape(1, n)
    gd, wd = row(gaia_dest), row(wise_dest)
    msg, places = send(gaia_pos, gaia_shape, row(gaia_corr), gd, row(gaia_cell), wise_pos, wise_shape, row(wise_corr), wd, row(wise_cell))
    ring = [[(i + ring_start(pix_count)) % pix_count for i in range(pix_count)]]
    exchange = lambda x: lax.all_to_all(x, "pix", 0, 0, axis_index_groups=ring, tiled=True)
    got = exchange(msg.reshape(peers, 1, 3 * LANES))
    chunks, rest, own, ranks = compact(got.reshape(3 * peers, LANES))
    gather = lambda x: lax.all_to_all(x, ("sub", "rep"), 0, 0, tiled=True).reshape(-1, LANES)
    near = gather(chunks)
    results, over = match(near, own, ranks)

    def with_rest():
        return match_whole(near, gather(jnp.broadcast_to(rest[None], (members, *rest.shape))), own, ranks)

    results = lax.cond(over[0, 0] > 0, with_rest, lambda: results)
    returned = exchange(results.reshape(peers, 1, LANES))
    like, offset, wise = back(returned.reshape(peers, LANES), places)
    return like.reshape(n), offset, wise.reshape(n)


def solution(mesh):
    flat = P(("groups", "pix", "sub", "rep"))
    pair = P(None, ("groups", "pix", "sub", "rep"))
    column = P(("groups", "pix", "sub", "rep"), None)
    return jax.shard_map(
        shards,
        mesh=mesh,
        in_specs=(pair, pair, flat, column, flat, pair, pair, flat, column, flat),
        out_specs=(flat, pair, flat),
        check_vma=False,
    )
```

```python
import math

import jax
import jax.numpy as jnp
from jax import lax
from jax.experimental import pallas as pl
from jax.experimental.pallas import tpu as pltpu
from jax.sharding import PartitionSpec as P

NCOL = 64
CAP = 2
LANES = 128
SLOT_LANES = 16
FIELDS = 8
EMPTY_BIT = 4096
ROW_BIT = 8192
LAMBDA = 2.0 * math.log(2.0)
GAIN = LAMBDA / (2.0 * math.pi)
GROUPS = 8
USED = 6
PART = 3
INTERPRET = False

f32 = jnp.float32
bf16 = jnp.bfloat16
i32 = jnp.int32


def iota(shape, dim):
    return lax.broadcasted_iota(i32, shape, dim)


def split3(x):
    high = x.astype(bf16)
    rest = x - high.astype(f32)
    middle = rest.astype(bf16)
    low = (rest - middle.astype(f32)).astype(bf16)
    return high, middle, low


def dot(a, b, contract):
    return lax.dot_general(a, b, (contract, ((), ())), preferred_element_type=f32)


def one_hot(mask):
    return jnp.where(mask, 1.0, 0.0).astype(bf16)


def call(body, outs, scratch=(), grant=8 << 20, **more):
    return pl.pallas_call(
        body,
        out_shape=outs,
        **more,
        scratch_shapes=list(scratch),
        compiler_params=pltpu.CompilerParams(vmem_limit_bytes=grant),
        interpret=INTERPRET,
    )


def ring_start(pix_count):
    return pix_count * 3 // 4


def part_rows():
    return -(-(PART * 2 * USED + 2) // 8) * 8


def tile_row(t, c):
    return t // PART * part_rows() + t % PART * 2 * USED + c * USED


def owners_and_ranks(dest_g, dest_w, sub_count):
    n = dest_g.shape[1]
    shift = sub_count.bit_length() - 1
    own_g, own_w = dest_g >> shift, dest_w >> shift
    both = jnp.concatenate([own_g.astype(f32), own_w.astype(f32), jnp.zeros((6, n), f32)], axis=0)
    columns = jnp.transpose(both)
    earlier = iota((n, n), 0) < iota((n, n), 1)

    def rank(row, column):
        same = (row.astype(f32) == column) & earlier
        return jnp.sum(jnp.where(same, 1.0, 0.0), axis=0, keepdims=True).astype(i32)

    return own_g, own_w, rank(own_g, columns[:, 0:1]), rank(own_w, columns[:, 1:2])


def send_body(pix_count, sub_count, peers):
    slots = CAP * sub_count
    turn = pix_count - ring_start(pix_count)

    def body(*refs):
        gp, gs, gc, gd, gl, wp, ws, wc, wd, wl, msg, places = refs
        n = gp.shape[1]
        own_g, own_w, rank_g, rank_w = owners_and_ranks(gd[...], wd[...], sub_count)

        def fields(pos, shape, corr, cell):
            a, b = shape[0:1, :], shape[1:2, :]
            return jnp.concatenate(
                [
                    pos[0:1, :],
                    pos[1:2, :],
                    (a * a) * LAMBDA,
                    (b * b) * LAMBDA,
                    ((corr * a) * b) * (2.0 * LAMBDA),
                    cell.astype(f32) + 1.0,
                    jnp.zeros((2, n), f32),
                ],
                axis=0,
            )

        data_g = fields(gp, gs, gc[...], gl[...])
        data_w = fields(wp, ws, wc[...], wl[...])
        zero = jnp.zeros((FIELDS, n), f32)
        left, right = [], []
        for s in range(slots):
            left += [jnp.where(rank_g == s, data_g, 0.0), zero]
            right += [zero, jnp.where(rank_w == s, data_w, 0.0)]
        table = jnp.concatenate([jnp.concatenate(left, axis=0), jnp.concatenate(right, axis=0)], axis=1)
        rows = 3 * peers
        r = iota((rows, 2 * n), 0)
        peer = jnp.floor((r.astype(f32) + 0.5) * (1.0 / 3.0)).astype(i32)
        side = r - 3 * peer
        band = (peer - turn) & (peers - 1)
        owner = jnp.concatenate([own_g, own_w], axis=1)
        upper = jnp.concatenate([gl[...], wl[...]], axis=1) >> (NCOL.bit_length() - 1)
        edge = (side == 1) | (upper == jnp.where(side == 0, 1, 0))
        pick = one_hot((owner == band + side - 1) & (band < pix_count) & edge)
        msg[...] = sum(dot(pick, part, ((1,), (1,))) for part in split3(table))
        at = [(o + turn) & (peers - 1) for o in (own_g, own_w)]
        places[...] = jnp.concatenate(at + [rank_g, rank_w, jnp.zeros((4, n), i32)], axis=0)

    return body


def compact_body(peers, slots, members, width):
    lanes = -(-3 * peers // LANES) * LANES
    tiles = width // LANES

    def body(got, out, rest, own, ranks, chunk):
        parts = [got[pl.ds(j, peers, stride=3), :] for j in (1, 0, 2)]
        parts.append(jnp.zeros((lanes - 3 * peers, LANES), f32))
        data = jnp.transpose(jnp.concatenate(parts, axis=0))
        lane8 = iota((FIELDS, lanes), 1)
        row8 = iota((FIELDS, lanes), 0)
        row_of = iota((FIELDS, LANES), 0)
        is_own = lane8 < peers
        is_low = (lane8 >= peers) & (lane8 < 2 * peers)
        before = one_hot(iota((lanes, lanes), 0) < iota((lanes, lanes), 1))
        below = one_hot(iota((slots, slots), 1) < iota((slots, slots), 0))
        goal = iota((LANES, lanes), 0).astype(f32)
        chunk[...] = jnp.zeros(chunk.shape, f32)
        own[...] = jnp.zeros(own.shape, f32)
        rank_rows, ready = [], []
        for c in range(2):
            pieces, codes = [], []
            for s in range(slots):
                x = data[s * SLOT_LANES + c * FIELDS : s * SLOT_LANES + (c + 1) * FIELDS, :]
                code = x[5:6, :]
                filled = code > 0.5
                cell = code.astype(i32) - 1
                row = jnp.where(is_own, cell >> 6, jnp.where(is_low, -1, 2)).astype(f32)
                away = jnp.where(is_own, 0, jnp.where(is_low, 512, 256))
                own_row = jnp.where(is_own, (cell >> 6) * ROW_BIT, 0)
                seen = ((cell & (NCOL - 1)) - away + EMPTY_BIT + own_row).astype(f32)
                x = jnp.where(row8 == 1, x + row, jnp.where(row8 == 5, seen, x))
                pieces.append(jnp.where(filled, x, 0.0))
                codes.append(code)
            filled = jnp.concatenate(codes, axis=0) > 0.5
            lane_s = iota((slots, lanes), 1)
            flag_own = jnp.where(filled & (lane_s < peers), 1.0, 0.0)
            flag_far = jnp.where(filled & (lane_s >= peers), 1.0, 0.0)

            def places(flag):
                inside = dot(flag.astype(bf16), before, ((1,), (0,)))
                totals = jnp.broadcast_to(jnp.sum(flag, axis=1, keepdims=True), (slots, LANES))
                ahead = dot(below, totals.astype(bf16), ((1,), (0,)))
                return inside + ahead[:, 0:1], jnp.sum(totals, axis=0, keepdims=True)

            place_own, count_own = places(flag_own)
            place_far, count_far = places(flag_far)
            place = jnp.where(flag_own > 0.5, place_own, place_far + count_own[:, 0:1])
            place = jnp.where(filled, place, -1.0)
            count = count_own + count_far
            rank_rows.append(place[:, 0:LANES])
            stacked = [jnp.concatenate(split3(p), axis=0) for p in pieces]
            total = jnp.max(count)
            chunk[PART * 2 * USED + c : PART * 2 * USED + c + 1, :] = count
            ready.append((place, stacked, count_own, total))

        def move(t, c):
            place, stacked, count_own, _ = ready[c]
            goal_t = goal + float(t * LANES)
            acc = jnp.zeros((3 * FIELDS, LANES), f32)
            for s in range(slots):
                pick = one_hot(goal_t == place[s : s + 1, :])
                acc = acc + dot(stacked[s], pick, ((1,), (1,)))
            x = acc[0:8, :] + acc[8:16, :] + acc[16:24, :]
            at = tile_row(t, c)
            chunk[at : at + USED, :] = x[0:USED, :]
            if t * LANES < own.shape[1]:
                x = jnp.where(row_of == 7, count_own, x)
                own[c * FIELDS : (c + 1) * FIELDS, t * LANES : (t + 1) * LANES] = x

        for t in range(PART):
            for c in range(2):
                move(t, c)

        @pl.when(jnp.maximum(ready[0][3], ready[1][3]) > PART * LANES)
        def _():
            for t in range(PART, tiles):
                for c in range(2):
                    move(t, c)

        ranks[...] = jnp.transpose(jnp.concatenate(rank_rows + [jnp.zeros((LANES - 2 * slots, LANES), f32)], axis=0))
        value = chunk[0 : part_rows(), :]
        for d in range(members):
            out[d] = value
        rest[...] = chunk[part_rows() :, :]

    return body


def prepare_body(peers, slots):
    used = 2 * USED

    def body(own, ranks, wide, pick):
        own_width = peers * slots
        stacked = jnp.concatenate([p.astype(f32) for p in split3(own[...])], axis=0)
        columns = jnp.transpose(stacked).astype(bf16)
        spread_to = iota((6 * FIELDS, used * LANES), 1) >> 7
        field_of = spread_to + jnp.where(spread_to >= USED, FIELDS - USED, 0)
        spread = one_hot((iota((6 * FIELDS, used * LANES), 0) & (2 * FIELDS - 1)) == field_of)
        wide[0:own_width, :] = dot(columns, spread, ((1,), (0,)))
        wide[own_width:, :] = jnp.zeros((8 * GROUPS, used * LANES), f32)
        goal = iota((peers, own_width), 1).astype(f32)
        for c in range(2):
            for s in range(slots):
                rank = ranks[0:peers, c * slots + s : c * slots + s + 1]
                pick[s * peers : (s + 1) * peers, c * own_width : (c + 1) * own_width] = one_hot(rank == goal)

    return body


def match_body(peers, slots, members, tiles):
    block = 8 * GROUPS
    whole = tiles > PART
    usual = PART
    rows = part_rows()
    own_width = peers * slots
    early = own_width * 3 // 4

    prepare = prepare_body(peers, slots)

    def body(*refs):
        near, refs = refs[: 1 + whole], refs[1 + whole :]
        own, ranks, out, refs = refs[0], refs[1], refs[2], refs[3:]
        over, refs = refs[: 1 - whole], refs[1 - whole :]
        wide, pick, line, totals, values = refs
        prepare(own, ranks, wide, pick)
        lane8 = iota((8, LANES), 1)
        count_own = [jnp.max(own[c * FIELDS + 7 : c * FIELDS + 8, 0:LANES]).astype(i32) for c in range(2)]

        def count_of(d, c):
            at = d * rows + PART * 2 * USED + c
            return jnp.max(near[0][at : at + 1, :]).astype(i32)

        counts = [[count_of(d, c) for d in range(members)] for c in range(2)]
        if not whole:
            most = counts[0][0]
            for n in counts[0][1:] + counts[1]:
                most = jnp.maximum(most, n)
            over[0][0, 0] = (most > PART * LANES).astype(i32)
            counts = [[jnp.minimum(n, PART * LANES) for n in line_counts] for line_counts in counts]
        ends = []
        for c in range(2):
            start = jnp.int32(0)
            for d in range(members):
                shift = start & (LANES - 1)
                base = start >> 7
                keep = lane8 >= shift

                def put(k, x, c=c, base=base):
                    line[c, base + k] = x

                def turned(k, c=c, d=d, shift=shift):
                    at = d * rows + tile_row(k % PART, c)
                    return pltpu.roll(near[k // PART][at : at + FIELDS, :], shift, 1)

                last = jnp.zeros((FIELDS, LANES), f32) if d == 0 else line[c, base]
                for k in range(usual):
                    now = turned(k)
                    put(k, jnp.where(keep, now, last))
                    last = now
                put(usual, jnp.where(keep, 0.0, last))
                put(usual + 1, jnp.zeros((FIELDS, LANES), f32))

                if not whole:
                    start = start + counts[c][d]
                    continue

                @pl.when(counts[c][d] > usual * LANES)
                def _(c=c, base=base, keep=keep, put=put, turned=turned):
                    last = line[c, base + usual]
                    for k in range(usual, tiles):
                        now = turned(k)
                        put(k, jnp.where(keep, now, last))
                        last = now
                    put(tiles, jnp.where(keep, 0.0, last))
                    put(tiles + 1, jnp.zeros((FIELDS, LANES), f32))

                start = start + counts[c][d]
            ends.append(lax.div(start + (2 * LANES - 1), 2 * LANES))

        for c in range(2):
            other = 1 - c
            blocks = lax.div(count_own[c] + (block - 1), block)

            def own_block(b, _, c=c, other=other):
                base = pl.multiple_of(b * block, 8)
                fields = []
                for g in range(GROUPS):
                    col = [wide[pl.ds(base + 8 * g, 8), (c * USED + f) * LANES : (c * USED + f + 1) * LANES] for f in range(USED)]
                    code = col[5].astype(i32)
                    own_code = code + (NCOL + 1 - EMPTY_BIT)
                    mask = jnp.where(code < ROW_BIT, 256, 512) | (EMPTY_BIT | (NCOL - 1))
                    fields.append((col[0] - 1.0, col[1], col[2], col[3], col[4], own_code, mask))

                def pairs(t, acc):
                    acc = [list(a) for a in acc]
                    for half in range(2):
                        at = line.at[other, 2 * t + half]
                        row = [jnp.broadcast_to(at[f : f + 1, :], (8, LANES)) for f in range(USED)]
                        code = row[5].astype(i32) - EMPTY_BIT
                        for g in range(GROUPS):
                            px, py, xx, yy, xy, own_code, mask = fields[g]
                            step = (own_code - code) & mask
                            dx = step.astype(f32) + (px - row[0])
                            dy = py - row[1]
                            sx, sy, sxy = xx + row[2], yy + row[3], xy + row[4]
                            det = sx * sy - 0.25 * (sxy * sxy)
                            root = lax.rsqrt(det)
                            chi = dy * (sxy * dx - sx * dy) - sy * (dx * dx)
                            like = jnp.exp2(chi * (root * root)) * root
                            like = jnp.where(step <= 2, like, 0.0)
                            acc[g][0] = acc[g][0] + like
                            if c == 0:
                                acc[g][1] = acc[g][1] + like * dx
                                acc[g][2] = acc[g][2] + like * dy
                    return tuple(tuple(a) for a in acc)

                zero = jnp.zeros((8, LANES), f32)
                acc = tuple((zero,) * (3 if c == 0 else 1) for _ in range(GROUPS))
                acc = lax.fori_loop(0, ends[other], pairs, acc)
                for g in range(GROUPS):
                    for k, a in enumerate(acc[g]):
                        totals[3 * c + k, pl.ds(base + 8 * g, 8), :] = a
                return 0

            lax.fori_loop(0, blocks, own_block, 0)

        f_of_lane = lane8 & (SLOT_LANES - 1)

        def sum_rows(first, last):
            for c in range(2):
                for g in range(first // 8, last // 8):
                    live = (iota((8, LANES), 0) + 8 * g) < count_own[c]
                    value = jnp.zeros((8, LANES), f32)
                    for k in range(3 if c == 0 else 1):
                        total = jnp.sum(totals[3 * c + k, 8 * g : 8 * g + 8, :], axis=1, keepdims=True) * GAIN
                        value = jnp.where(f_of_lane == c * FIELDS + k, total, value)
                    values[c * own_width + 8 * g : c * own_width + 8 * g + 8, :] = jnp.where(live, value, 0.0)

        many = jnp.maximum(count_own[0], count_own[1]) > early
        sum_rows(0, early)

        @pl.when(many)
        def _():
            sum_rows(early, own_width)

        @pl.when(jnp.logical_not(many))
        def _():
            for c in range(2):
                values[c * own_width + early : (c + 1) * own_width, :] = jnp.zeros((own_width - early, LANES), f32)

        result = sum(dot(pick[...], part, ((1,), (0,))) for part in split3(values[...])[:2])
        slot_of_lane = iota((peers, LANES), 1) >> 4
        final = jnp.zeros((peers, LANES), f32)
        for s in range(slots):
            final = final + jnp.where(slot_of_lane == s, result[s * peers : (s + 1) * peers, :], 0.0)
        out[...] = final

    return body


def return_body(sub_count, peers):
    slots = CAP * sub_count

    def body(back, places, like, offset, wise):
        n = places.shape[1]
        at = jnp.concatenate([places[0:1, :], places[1:2, :]], axis=1)
        rank_g, rank_w = places[2:3, :], places[3:4, :]
        pick = one_hot(iota((peers, 2 * n), 0) == at)
        turned = jnp.transpose(back[...])
        found = sum(dot(part, pick, ((1,), (0,))) for part in split3(turned)[:2])
        gaia = jnp.zeros((FIELDS, n), f32)
        other = jnp.zeros((FIELDS, n), f32)
        for s in range(slots):
            at = s * SLOT_LANES
            gaia = gaia + jnp.where(rank_g == s, found[at : at + FIELDS, 0:n], 0.0)
            other = other + jnp.where(rank_w == s, found[at + FIELDS : at + 2 * FIELDS, n : 2 * n], 0.0)
        like[...] = gaia[0:1, :]
        offset[...] = gaia[1:3, :]
        wise[...] = other[0:1, :]

    return body


def stages(pix_count, sub_count, rep_count, n):
    peers = pix_count
    members = sub_count * rep_count
    slots = CAP * sub_count
    width = 3 * peers * slots
    own_width = peers * slots
    rows = part_rows()
    parts = width // LANES // PART
    pair, line, whole = pltpu.VMEM((2, n), f32), pltpu.VMEM((1, n), f32), pltpu.VMEM((1, n), i32)
    send = call(
        send_body(pix_count, sub_count, peers),
        (jax.ShapeDtypeStruct((3 * peers, LANES), f32), jax.ShapeDtypeStruct((8, n), i32)),
    )
    compact = call(
        compact_body(peers, slots, members, width),
        (
            jax.ShapeDtypeStruct((members, rows, LANES), f32),
            jax.ShapeDtypeStruct(((parts - 1) * rows, LANES), f32),
            jax.ShapeDtypeStruct((2 * FIELDS, own_width), f32),
            jax.ShapeDtypeStruct((LANES, LANES), f32),
        ),
        [pltpu.VMEM((parts * rows, LANES), f32)],
    )
    results = jax.ShapeDtypeStruct((peers, LANES), f32)
    held = lambda tiles: [
        pltpu.VMEM((own_width + 8 * GROUPS, 2 * USED * LANES), f32),
        pltpu.VMEM((own_width, 2 * own_width), bf16),
        pltpu.VMEM((2, members * tiles + 8, FIELDS, LANES), f32),
        pltpu.VMEM((4, own_width + 8 * GROUPS, LANES), f32),
        pltpu.VMEM((2 * own_width, LANES), f32),
    ]
    match = call(
        match_body(peers, slots, members, PART),
        (results, jax.ShapeDtypeStruct((1, 1), i32)),
        held(PART),
        out_specs=(pl.BlockSpec(memory_space=pltpu.VMEM), pl.BlockSpec(memory_space=pltpu.SMEM)),
    )
    match_whole = call(match_body(peers, slots, members, width // LANES), results, held(width // LANES))
    back = call(
        return_body(sub_count, peers),
        (
            jax.ShapeDtypeStruct((1, n), f32),
            jax.ShapeDtypeStruct((2, n), f32),
            jax.ShapeDtypeStruct((1, n), f32),
        ),
    )
    return send, compact, match, match_whole, back


def shards(gaia_pos, gaia_shape, gaia_corr, gaia_dest, gaia_cell, wise_pos, wise_shape, wise_corr, wise_dest, wise_cell):
    pix_count = lax.axis_size("pix")
    sub_count = lax.axis_size("sub")
    rep_count = lax.axis_size("rep")
    peers = pix_count
    members = sub_count * rep_count
    n = gaia_pos.shape[1]
    send, compact, match, match_whole, back = stages(pix_count, sub_count, rep_count, n)
    row = lambda x: x.reshape(1, n)
    gd, wd = row(gaia_dest), row(wise_dest)
    msg, places = send(gaia_pos, gaia_shape, row(gaia_corr), gd, row(gaia_cell), wise_pos, wise_shape, row(wise_corr), wd, row(wise_cell))
    ring = [[(i + ring_start(pix_count)) % pix_count for i in range(pix_count)]]
    exchange = lambda x: lax.all_to_all(x, "pix", 0, 0, axis_index_groups=ring, tiled=True)
    got = exchange(msg.reshape(peers, 1, 3 * LANES))
    chunks, rest, own, ranks = compact(got.reshape(3 * peers, LANES))
    gather = lambda x: lax.all_to_all(x, ("sub", "rep"), 0, 0, tiled=True).reshape(-1, LANES)
    near = gather(chunks)
    results, over = match(near, own, ranks)

    def with_rest():
        return match_whole(near, gather(jnp.broadcast_to(rest[None], (members, *rest.shape))), own, ranks)

    results = lax.cond(over[0, 0] > 0, with_rest, lambda: results)
    returned = exchange(results.reshape(peers, 1, LANES))
    like, offset, wise = back(returned.reshape(peers, LANES), places)
    return like.reshape(n), offset, wise.reshape(n)


def solution(mesh):
    flat = P(("groups", "pix", "sub", "rep"))
    pair = P(None, ("groups", "pix", "sub", "rep"))
    column = P(("groups", "pix", "sub", "rep"), None)
    return jax.shard_map(
        shards,
        mesh=mesh,
        in_specs=(pair, pair, flat, column, flat, pair, pair, flat, column, flat),
        out_specs=(flat, pair, flat),
        check_vma=False,
    )
```

```python
import math

import jax
import jax.numpy as jnp
from jax import lax
from jax.experimental import pallas as pl
from jax.experimental.pallas import tpu as pltpu
from jax.sharding import PartitionSpec as P

NCOL = 64
CAP = 2
LANES = 128
SLOT_LANES = 16
FIELDS = 8
EMPTY_BIT = 4096
ROW_BIT = 8192
LAMBDA = 2.0 * math.log(2.0)
GAIN = LAMBDA / (2.0 * math.pi)
GROUPS = 8
USED = 6
PART = 3
INTERPRET = False

f32 = jnp.float32
bf16 = jnp.bfloat16
i32 = jnp.int32


def iota(shape, dim):
    return lax.broadcasted_iota(i32, shape, dim)


def split3(x):
    high = x.astype(bf16)
    rest = x - high.astype(f32)
    middle = rest.astype(bf16)
    low = (rest - middle.astype(f32)).astype(bf16)
    return high, middle, low


def dot(a, b, contract):
    return lax.dot_general(a, b, (contract, ((), ())), preferred_element_type=f32)


def one_hot(mask):
    return jnp.where(mask, 1.0, 0.0).astype(bf16)


def call(body, outs, scratch=(), grant=8 << 20, **more):
    return pl.pallas_call(
        body,
        out_shape=outs,
        **more,
        scratch_shapes=list(scratch),
        compiler_params=pltpu.CompilerParams(vmem_limit_bytes=grant),
        interpret=INTERPRET,
    )


def ring_start(pix_count):
    return pix_count * 5 // 8


def part_rows():
    return -(-(PART * 2 * USED + 2) // 8) * 8


def tile_row(t, c):
    return t // PART * part_rows() + t % PART * 2 * USED + c * USED


def owners_and_ranks(dest_g, dest_w, sub_count):
    n = dest_g.shape[1]
    shift = sub_count.bit_length() - 1
    own_g, own_w = dest_g >> shift, dest_w >> shift
    both = jnp.concatenate([own_g.astype(f32), own_w.astype(f32), jnp.zeros((6, n), f32)], axis=0)
    columns = jnp.transpose(both)
    earlier = iota((n, n), 0) < iota((n, n), 1)

    def rank(row, column):
        same = (row.astype(f32) == column) & earlier
        return jnp.sum(jnp.where(same, 1.0, 0.0), axis=0, keepdims=True).astype(i32)

    return own_g, own_w, rank(own_g, columns[:, 0:1]), rank(own_w, columns[:, 1:2])


def send_body(pix_count, sub_count, peers):
    slots = CAP * sub_count
    turn = pix_count - ring_start(pix_count)

    def body(*refs):
        gp, gs, gc, gd, gl, wp, ws, wc, wd, wl, msg, places = refs
        n = gp.shape[1]
        own_g, own_w, rank_g, rank_w = owners_and_ranks(gd[...], wd[...], sub_count)

        def fields(pos, shape, corr, cell):
            a, b = shape[0:1, :], shape[1:2, :]
            return jnp.concatenate(
                [
                    pos[0:1, :],
                    pos[1:2, :],
                    (a * a) * LAMBDA,
                    (b * b) * LAMBDA,
                    ((corr * a) * b) * (2.0 * LAMBDA),
                    cell.astype(f32) + 1.0,
                    jnp.zeros((2, n), f32),
                ],
                axis=0,
            )

        data_g = fields(gp, gs, gc[...], gl[...])
        data_w = fields(wp, ws, wc[...], wl[...])
        zero = jnp.zeros((FIELDS, n), f32)
        left, right = [], []
        for s in range(slots):
            left += [jnp.where(rank_g == s, data_g, 0.0), zero]
            right += [zero, jnp.where(rank_w == s, data_w, 0.0)]
        table = jnp.concatenate([jnp.concatenate(left, axis=0), jnp.concatenate(right, axis=0)], axis=1)
        rows = 3 * peers
        r = iota((rows, 2 * n), 0)
        peer = jnp.floor((r.astype(f32) + 0.5) * (1.0 / 3.0)).astype(i32)
        side = r - 3 * peer
        band = (peer - turn) & (peers - 1)
        owner = jnp.concatenate([own_g, own_w], axis=1)
        upper = jnp.concatenate([gl[...], wl[...]], axis=1) >> (NCOL.bit_length() - 1)
        edge = (side == 1) | (upper == jnp.where(side == 0, 1, 0))
        pick = one_hot((owner == band + side - 1) & (band < pix_count) & edge)
        msg[...] = sum(dot(pick, part, ((1,), (1,))) for part in split3(table))
        at = [(o + turn) & (peers - 1) for o in (own_g, own_w)]
        places[...] = jnp.concatenate(at + [rank_g, rank_w, jnp.zeros((4, n), i32)], axis=0)

    return body


def compact_body(peers, slots, members, width):
    lanes = -(-3 * peers // LANES) * LANES
    tiles = width // LANES

    def body(got, out, rest, own, ranks, chunk):
        parts = [got[pl.ds(j, peers, stride=3), :] for j in (1, 0, 2)]
        parts.append(jnp.zeros((lanes - 3 * peers, LANES), f32))
        data = jnp.transpose(jnp.concatenate(parts, axis=0))
        lane8 = iota((FIELDS, lanes), 1)
        row8 = iota((FIELDS, lanes), 0)
        row_of = iota((FIELDS, LANES), 0)
        is_own = lane8 < peers
        is_low = (lane8 >= peers) & (lane8 < 2 * peers)
        before = one_hot(iota((lanes, lanes), 0) < iota((lanes, lanes), 1))
        below = one_hot(iota((slots, slots), 1) < iota((slots, slots), 0))
        goal = iota((LANES, lanes), 0).astype(f32)
        chunk[...] = jnp.zeros(chunk.shape, f32)
        own[...] = jnp.zeros(own.shape, f32)
        rank_rows, ready = [], []
        for c in range(2):
            pieces, codes = [], []
            for s in range(slots):
                x = data[s * SLOT_LANES + c * FIELDS : s * SLOT_LANES + (c + 1) * FIELDS, :]
                code = x[5:6, :]
                filled = code > 0.5
                cell = code.astype(i32) - 1
                row = jnp.where(is_own, cell >> 6, jnp.where(is_low, -1, 2)).astype(f32)
                away = jnp.where(is_own, 0, jnp.where(is_low, 512, 256))
                own_row = jnp.where(is_own, (cell >> 6) * ROW_BIT, 0)
                seen = ((cell & (NCOL - 1)) - away + EMPTY_BIT + own_row).astype(f32)
                x = jnp.where(row8 == 1, x + row, jnp.where(row8 == 5, seen, x))
                pieces.append(jnp.where(filled, x, 0.0))
                codes.append(code)
            filled = jnp.concatenate(codes, axis=0) > 0.5
            lane_s = iota((slots, lanes), 1)
            flag_own = jnp.where(filled & (lane_s < peers), 1.0, 0.0)
            flag_far = jnp.where(filled & (lane_s >= peers), 1.0, 0.0)

            def places(flag):
                inside = dot(flag.astype(bf16), before, ((1,), (0,)))
                totals = jnp.broadcast_to(jnp.sum(flag, axis=1, keepdims=True), (slots, LANES))
                ahead = dot(below, totals.astype(bf16), ((1,), (0,)))
                return inside + ahead[:, 0:1], jnp.sum(totals, axis=0, keepdims=True)

            place_own, count_own = places(flag_own)
            place_far, count_far = places(flag_far)
            place = jnp.where(flag_own > 0.5, place_own, place_far + count_own[:, 0:1])
            place = jnp.where(filled, place, -1.0)
            count = count_own + count_far
            rank_rows.append(place[:, 0:LANES])
            stacked = [jnp.concatenate(split3(p), axis=0) for p in pieces]
            total = jnp.max(count)
            chunk[PART * 2 * USED + c : PART * 2 * USED + c + 1, :] = count
            ready.append((place, stacked, count_own, total))

        def move(t, c):
            place, stacked, count_own, _ = ready[c]
            goal_t = goal + float(t * LANES)
            acc = jnp.zeros((3 * FIELDS, LANES), f32)
            for s in range(slots):
                pick = one_hot(goal_t == place[s : s + 1, :])
                acc = acc + dot(stacked[s], pick, ((1,), (1,)))
            x = acc[0:8, :] + acc[8:16, :] + acc[16:24, :]
            at = tile_row(t, c)
            chunk[at : at + USED, :] = x[0:USED, :]
            if t * LANES < own.shape[1]:
                x = jnp.where(row_of == 7, count_own, x)
                own[c * FIELDS : (c + 1) * FIELDS, t * LANES : (t + 1) * LANES] = x

        for t in range(PART):
            for c in range(2):
                move(t, c)

        @pl.when(jnp.maximum(ready[0][3], ready[1][3]) > PART * LANES)
        def _():
            for t in range(PART, tiles):
                for c in range(2):
                    move(t, c)

        ranks[...] = jnp.transpose(jnp.concatenate(rank_rows + [jnp.zeros((LANES - 2 * slots, LANES), f32)], axis=0))
        value = chunk[0 : part_rows(), :]
        for d in range(members):
            out[d] = value
        rest[...] = chunk[part_rows() :, :]

    return body


def prepare_body(peers, slots):
    used = 2 * USED

    def body(own, ranks, wide, pick):
        own_width = peers * slots
        stacked = jnp.concatenate([p.astype(f32) for p in split3(own[...])], axis=0)
        columns = jnp.transpose(stacked).astype(bf16)
        spread_to = iota((6 * FIELDS, used * LANES), 1) >> 7
        field_of = spread_to + jnp.where(spread_to >= USED, FIELDS - USED, 0)
        spread = one_hot((iota((6 * FIELDS, used * LANES), 0) & (2 * FIELDS - 1)) == field_of)
        wide[...] = dot(columns, spread, ((1,), (0,)))
        goal = iota((peers, own_width), 1).astype(f32)
        for c in range(2):
            for s in range(slots):
                rank = ranks[0:peers, c * slots + s : c * slots + s + 1]
                pick[s * peers : (s + 1) * peers, c * own_width : (c + 1) * own_width] = one_hot(rank == goal)

    return body


def match_body(peers, slots, members, tiles):
    block = 8 * GROUPS
    whole = tiles > PART
    usual = PART
    rows = part_rows()
    own_width = peers * slots
    early = own_width * 3 // 4

    prepare = prepare_body(peers, slots)

    def body(*refs):
        near, refs = refs[: 1 + whole], refs[1 + whole :]
        own, ranks, out, refs = refs[0], refs[1], refs[2], refs[3:]
        over, refs = refs[: 1 - whole], refs[1 - whole :]
        wide, pick, line, totals, values = refs
        prepare(own, ranks, wide, pick)
        lane8 = iota((8, LANES), 1)
        count_own = [jnp.max(own[c * FIELDS + 7 : c * FIELDS + 8, 0:LANES]).astype(i32) for c in range(2)]

        def count_of(d, c):
            at = d * rows + PART * 2 * USED + c
            return jnp.max(near[0][at : at + 1, :]).astype(i32)

        counts = [[count_of(d, c) for d in range(members)] for c in range(2)]
        if not whole:
            most = counts[0][0]
            for n in counts[0][1:] + counts[1]:
                most = jnp.maximum(most, n)
            over[0][0, 0] = (most > PART * LANES).astype(i32)
            counts = [[jnp.minimum(n, PART * LANES) for n in line_counts] for line_counts in counts]
        ends = []
        for c in range(2):
            start = jnp.int32(0)
            for d in range(members):
                shift = start & (LANES - 1)
                base = start >> 7
                keep = lane8 >= shift

                def put(k, x, c=c, base=base):
                    line[c, base + k] = x

                def turned(k, c=c, d=d, shift=shift):
                    at = d * rows + tile_row(k % PART, c)
                    return pltpu.roll(near[k // PART][at : at + FIELDS, :], shift, 1)

                last = jnp.zeros((FIELDS, LANES), f32) if d == 0 else line[c, base]
                for k in range(usual):
                    now = turned(k)
                    put(k, jnp.where(keep, now, last))
                    last = now
                put(usual, jnp.where(keep, 0.0, last))
                put(usual + 1, jnp.zeros((FIELDS, LANES), f32))

                if not whole:
                    start = start + counts[c][d]
                    continue

                @pl.when(counts[c][d] > usual * LANES)
                def _(c=c, base=base, keep=keep, put=put, turned=turned):
                    last = line[c, base + usual]
                    for k in range(usual, tiles):
                        now = turned(k)
                        put(k, jnp.where(keep, now, last))
                        last = now
                    put(tiles, jnp.where(keep, 0.0, last))
                    put(tiles + 1, jnp.zeros((FIELDS, LANES), f32))

                start = start + counts[c][d]
            ends.append(lax.div(start + (2 * LANES - 1), 2 * LANES))

        for c in range(2):
            other = 1 - c
            blocks = lax.div(count_own[c] + (block - 1), block)

            def own_block(b, _, c=c, other=other):
                base = pl.multiple_of(b * block, 8)
                fields = []
                for g in range(GROUPS):
                    col = [wide[pl.ds(base + 8 * g, 8), (c * USED + f) * LANES : (c * USED + f + 1) * LANES] for f in range(USED)]
                    code = col[5].astype(i32)
                    own_code = code + (NCOL + 1 - EMPTY_BIT)
                    mask = jnp.where(code < ROW_BIT, 256, 512) | (EMPTY_BIT | (NCOL - 1))
                    fields.append((col[0] - 1.0, col[1], col[2], col[3], col[4], own_code, mask))

                def pairs(t, acc):
                    acc = [list(a) for a in acc]
                    for half in range(2):
                        at = line.at[other, 2 * t + half]
                        row = [jnp.broadcast_to(at[f : f + 1, :], (8, LANES)) for f in range(USED)]
                        code = row[5].astype(i32) - EMPTY_BIT
                        for g in range(GROUPS):
                            px, py, xx, yy, xy, own_code, mask = fields[g]
                            step = (own_code - code) & mask
                            dx = step.astype(f32) + (px - row[0])
                            dy = py - row[1]
                            sx, sy, sxy = xx + row[2], yy + row[3], xy + row[4]
                            det = sx * sy - 0.25 * (sxy * sxy)
                            root = lax.rsqrt(det)
                            chi = dy * (sxy * dx - sx * dy) - sy * (dx * dx)
                            like = jnp.exp2(chi * (root * root)) * root
                            like = jnp.where(step <= 2, like, 0.0)
                            acc[g][0] = acc[g][0] + like
                            if c == 0:
                                acc[g][1] = acc[g][1] + like * dx
                                acc[g][2] = acc[g][2] + like * dy
                    return tuple(tuple(a) for a in acc)

                zero = jnp.zeros((8, LANES), f32)
                acc = tuple((zero,) * (3 if c == 0 else 1) for _ in range(GROUPS))
                acc = lax.fori_loop(0, ends[other], pairs, acc)
                for g in range(GROUPS):
                    for k, a in enumerate(acc[g]):
                        totals[3 * c + k, pl.ds(base + 8 * g, 8), :] = a
                return 0

            lax.fori_loop(0, blocks, own_block, 0)

        f_of_lane = lane8 & (SLOT_LANES - 1)

        def sum_rows(first, last):
            for c in range(2):
                for g in range(first // 8, last // 8):
                    live = (iota((8, LANES), 0) + 8 * g) < count_own[c]
                    value = jnp.zeros((8, LANES), f32)
                    for k in range(3 if c == 0 else 1):
                        total = jnp.sum(totals[3 * c + k, 8 * g : 8 * g + 8, :], axis=1, keepdims=True) * GAIN
                        value = jnp.where(f_of_lane == c * FIELDS + k, total, value)
                    values[c * own_width + 8 * g : c * own_width + 8 * g + 8, :] = jnp.where(live, value, 0.0)

        many = jnp.maximum(count_own[0], count_own[1]) > early
        sum_rows(0, early)

        @pl.when(many)
        def _():
            sum_rows(early, own_width)

        @pl.when(jnp.logical_not(many))
        def _():
            for c in range(2):
                values[c * own_width + early : (c + 1) * own_width, :] = jnp.zeros((own_width - early, LANES), f32)

        result = sum(dot(pick[...], part, ((1,), (0,))) for part in split3(values[...])[:2])
        slot_of_lane = iota((peers, LANES), 1) >> 4
        final = jnp.zeros((peers, LANES), f32)
        for s in range(slots):
            final = final + jnp.where(slot_of_lane == s, result[s * peers : (s + 1) * peers, :], 0.0)
        out[...] = final

    return body


def return_body(sub_count, peers):
    slots = CAP * sub_count

    def body(back, places, like, offset, wise):
        n = places.shape[1]
        at = jnp.concatenate([places[0:1, :], places[1:2, :]], axis=1)
        rank_g, rank_w = places[2:3, :], places[3:4, :]
        pick = one_hot(iota((peers, 2 * n), 0) == at)
        turned = jnp.transpose(back[...])
        found = sum(dot(part, pick, ((1,), (0,))) for part in split3(turned)[:2])
        gaia = jnp.zeros((FIELDS, n), f32)
        other = jnp.zeros((FIELDS, n), f32)
        for s in range(slots):
            at = s * SLOT_LANES
            gaia = gaia + jnp.where(rank_g == s, found[at : at + FIELDS, 0:n], 0.0)
            other = other + jnp.where(rank_w == s, found[at + FIELDS : at + 2 * FIELDS, n : 2 * n], 0.0)
        like[...] = gaia[0:1, :]
        offset[...] = gaia[1:3, :]
        wise[...] = other[0:1, :]

    return body


def stages(pix_count, sub_count, rep_count, n):
    peers = pix_count
    members = sub_count * rep_count
    slots = CAP * sub_count
    width = 3 * peers * slots
    own_width = peers * slots
    rows = part_rows()
    parts = width // LANES // PART
    pair, line, whole = pltpu.VMEM((2, n), f32), pltpu.VMEM((1, n), f32), pltpu.VMEM((1, n), i32)
    send = call(
        send_body(pix_count, sub_count, peers),
        (jax.ShapeDtypeStruct((3 * peers, LANES), f32), jax.ShapeDtypeStruct((8, n), i32)),
    )
    compact = call(
        compact_body(peers, slots, members, width),
        (
            jax.ShapeDtypeStruct((members, rows, LANES), f32),
            jax.ShapeDtypeStruct(((parts - 1) * rows, LANES), f32),
            jax.ShapeDtypeStruct((2 * FIELDS, own_width), f32),
            jax.ShapeDtypeStruct((LANES, LANES), f32),
        ),
        [pltpu.VMEM((parts * rows, LANES), f32)],
    )
    results = jax.ShapeDtypeStruct((peers, LANES), f32)
    held = lambda tiles: [
        pltpu.VMEM((own_width, 2 * USED * LANES), f32),
        pltpu.VMEM((own_width, 2 * own_width), bf16),
        pltpu.VMEM((2, members * tiles + 8, FIELDS, LANES), f32),
        pltpu.VMEM((4, own_width, LANES), f32),
        pltpu.VMEM((2 * own_width, LANES), f32),
    ]
    match = call(
        match_body(peers, slots, members, PART),
        (results, jax.ShapeDtypeStruct((1, 1), i32)),
        held(PART),
        out_specs=(pl.BlockSpec(memory_space=pltpu.VMEM), pl.BlockSpec(memory_space=pltpu.SMEM)),
    )
    match_whole = call(match_body(peers, slots, members, width // LANES), results, held(width // LANES))
    back = call(
        return_body(sub_count, peers),
        (
            jax.ShapeDtypeStruct((1, n), f32),
            jax.ShapeDtypeStruct((2, n), f32),
            jax.ShapeDtypeStruct((1, n), f32),
        ),
    )
    return send, compact, match, match_whole, back


def shards(gaia_pos, gaia_shape, gaia_corr, gaia_dest, gaia_cell, wise_pos, wise_shape, wise_corr, wise_dest, wise_cell):
    pix_count = lax.axis_size("pix")
    sub_count = lax.axis_size("sub")
    rep_count = lax.axis_size("rep")
    peers = pix_count
    members = sub_count * rep_count
    n = gaia_pos.shape[1]
    send, compact, match, match_whole, back = stages(pix_count, sub_count, rep_count, n)
    row = lambda x: x.reshape(1, n)
    gd, wd = row(gaia_dest), row(wise_dest)
    msg, places = send(gaia_pos, gaia_shape, row(gaia_corr), gd, row(gaia_cell), wise_pos, wise_shape, row(wise_corr), wd, row(wise_cell))
    ring = [[(i + ring_start(pix_count)) % pix_count for i in range(pix_count)]]
    exchange = lambda x: lax.all_to_all(x, "pix", 0, 0, axis_index_groups=ring, tiled=True)
    got = exchange(msg.reshape(peers, 1, 3 * LANES))
    chunks, rest, own, ranks = compact(got.reshape(3 * peers, LANES))
    gather = lambda x: lax.all_to_all(x, ("rep", "sub"), 0, 0, tiled=True).reshape(-1, LANES)
    near = gather(chunks)
    results, over = match(near, own, ranks)

    def with_rest():
        return match_whole(near, gather(jnp.broadcast_to(rest[None], (members, *rest.shape))), own, ranks)

    results = lax.cond(over[0, 0] > 0, with_rest, lambda: results)
    returned = exchange(results.reshape(peers, 1, LANES))
    like, offset, wise = back(returned.reshape(peers, LANES), places)
    return like.reshape(n), offset, wise.reshape(n)


def solution(mesh):
    flat = P(("groups", "pix", "sub", "rep"))
    pair = P(None, ("groups", "pix", "sub", "rep"))
    column = P(("groups", "pix", "sub", "rep"), None)
    return jax.shard_map(
        shards,
        mesh=mesh,
        in_specs=(pair, pair, flat, column, flat, pair, pair, flat, column, flat),
        out_specs=(flat, pair, flat),
        check_vma=False,
    )
```

```python
import math

import jax
import jax.numpy as jnp
from jax import lax
from jax.experimental import pallas as pl
from jax.experimental.pallas import tpu as pltpu
from jax.sharding import PartitionSpec as P

NCOL = 64
CAP = 2
LANES = 128
SLOT_LANES = 16
FIELDS = 8
EMPTY_BIT = 4096
ROW_BIT = 8192
LAMBDA = 2.0 * math.log(2.0)
GAIN = LAMBDA / (2.0 * math.pi)
GROUPS = 8
USED = 6
PART = 3
INTERPRET = False

f32 = jnp.float32
bf16 = jnp.bfloat16
i32 = jnp.int32


def iota(shape, dim):
    return lax.broadcasted_iota(i32, shape, dim)


def split3(x):
    high = x.astype(bf16)
    rest = x - high.astype(f32)
    middle = rest.astype(bf16)
    low = (rest - middle.astype(f32)).astype(bf16)
    return high, middle, low


def dot(a, b, contract):
    return lax.dot_general(a, b, (contract, ((), ())), preferred_element_type=f32)


def one_hot(mask):
    return jnp.where(mask, 1.0, 0.0).astype(bf16)


def call(body, outs, scratch=(), grant=8 << 20, **more):
    return pl.pallas_call(
        body,
        out_shape=outs,
        **more,
        scratch_shapes=list(scratch),
        compiler_params=pltpu.CompilerParams(vmem_limit_bytes=grant),
        interpret=INTERPRET,
    )


def ring_start(pix_count):
    return pix_count // 2


def part_rows():
    return -(-(PART * 2 * USED + 2) // 8) * 8


def tile_row(t, c):
    return t // PART * part_rows() + t % PART * 2 * USED + c * USED


def owners_and_ranks(dest_g, dest_w, sub_count):
    n = dest_g.shape[1]
    shift = sub_count.bit_length() - 1
    own_g, own_w = dest_g >> shift, dest_w >> shift
    both = jnp.concatenate([own_g.astype(f32), own_w.astype(f32), jnp.zeros((6, n), f32)], axis=0)
    columns = jnp.transpose(both)
    earlier = iota((n, n), 0) < iota((n, n), 1)

    def rank(row, column):
        same = (row.astype(f32) == column) & earlier
        return jnp.sum(jnp.where(same, 1.0, 0.0), axis=0, keepdims=True).astype(i32)

    return own_g, own_w, rank(own_g, columns[:, 0:1]), rank(own_w, columns[:, 1:2])


def send_body(pix_count, sub_count, peers):
    slots = CAP * sub_count
    turn = pix_count - ring_start(pix_count)

    def body(*refs):
        gp, gs, gc, gd, gl, wp, ws, wc, wd, wl, msg, places = refs
        n = gp.shape[1]
        own_g, own_w, rank_g, rank_w = owners_and_ranks(gd[...], wd[...], sub_count)

        def fields(pos, shape, corr, cell):
            a, b = shape[0:1, :], shape[1:2, :]
            return jnp.concatenate(
                [
                    pos[0:1, :],
                    pos[1:2, :],
                    (a * a) * LAMBDA,
                    (b * b) * LAMBDA,
                    ((corr * a) * b) * (2.0 * LAMBDA),
                    cell.astype(f32) + 1.0,
                    jnp.zeros((2, n), f32),
                ],
                axis=0,
            )

        data_g = fields(gp, gs, gc[...], gl[...])
        data_w = fields(wp, ws, wc[...], wl[...])
        zero = jnp.zeros((FIELDS, n), f32)
        left, right = [], []
        for s in range(slots):
            left += [jnp.where(rank_g == s, data_g, 0.0), zero]
            right += [zero, jnp.where(rank_w == s, data_w, 0.0)]
        table = jnp.concatenate([jnp.concatenate(left, axis=0), jnp.concatenate(right, axis=0)], axis=1)
        rows = 3 * peers
        r = iota((rows, 2 * n), 0)
        peer = jnp.floor((r.astype(f32) + 0.5) * (1.0 / 3.0)).astype(i32)
        side = r - 3 * peer
        band = (peer - turn) & (peers - 1)
        owner = jnp.concatenate([own_g, own_w], axis=1)
        upper = jnp.concatenate([gl[...], wl[...]], axis=1) >> (NCOL.bit_length() - 1)
        edge = (side == 1) | (upper == jnp.where(side == 0, 1, 0))
        pick = one_hot((owner == band + side - 1) & (band < pix_count) & edge)
        msg[...] = sum(dot(pick, part, ((1,), (1,))) for part in split3(table))
        at = [(o + turn) & (peers - 1) for o in (own_g, own_w)]
        places[...] = jnp.concatenate(at + [rank_g, rank_w, jnp.zeros((4, n), i32)], axis=0)

    return body


def compact_body(peers, slots, members, width):
    lanes = -(-3 * peers // LANES) * LANES
    tiles = width // LANES

    def body(got, out, rest, own, ranks, chunk):
        parts = [got[pl.ds(j, peers, stride=3), :] for j in (1, 0, 2)]
        parts.append(jnp.zeros((lanes - 3 * peers, LANES), f32))
        data = jnp.transpose(jnp.concatenate(parts, axis=0))
        lane8 = iota((FIELDS, lanes), 1)
        row8 = iota((FIELDS, lanes), 0)
        row_of = iota((FIELDS, LANES), 0)
        is_own = lane8 < peers
        is_low = (lane8 >= peers) & (lane8 < 2 * peers)
        before = one_hot(iota((lanes, lanes), 0) < iota((lanes, lanes), 1))
        below = one_hot(iota((slots, slots), 1) < iota((slots, slots), 0))
        goal = iota((LANES, lanes), 0).astype(f32)
        chunk[...] = jnp.zeros(chunk.shape, f32)
        own[...] = jnp.zeros(own.shape, f32)
        rank_rows, ready = [], []
        for c in range(2):
            pieces, codes = [], []
            for s in range(slots):
                x = data[s * SLOT_LANES + c * FIELDS : s * SLOT_LANES + (c + 1) * FIELDS, :]
                code = x[5:6, :]
                filled = code > 0.5
                cell = code.astype(i32) - 1
                row = jnp.where(is_own, cell >> 6, jnp.where(is_low, -1, 2)).astype(f32)
                away = jnp.where(is_own, 0, jnp.where(is_low, 512, 256))
                own_row = jnp.where(is_own, (cell >> 6) * ROW_BIT, 0)
                seen = ((cell & (NCOL - 1)) - away + EMPTY_BIT + own_row).astype(f32)
                x = jnp.where(row8 == 1, x + row, jnp.where(row8 == 5, seen, x))
                pieces.append(jnp.where(filled, x, 0.0))
                codes.append(code)
            filled = jnp.concatenate(codes, axis=0) > 0.5
            lane_s = iota((slots, lanes), 1)
            flag_own = jnp.where(filled & (lane_s < peers), 1.0, 0.0)
            flag_far = jnp.where(filled & (lane_s >= peers), 1.0, 0.0)

            def places(flag):
                inside = dot(flag.astype(bf16), before, ((1,), (0,)))
                totals = jnp.broadcast_to(jnp.sum(flag, axis=1, keepdims=True), (slots, LANES))
                ahead = dot(below, totals.astype(bf16), ((1,), (0,)))
                return inside + ahead[:, 0:1], jnp.sum(totals, axis=0, keepdims=True)

            place_own, count_own = places(flag_own)
            place_far, count_far = places(flag_far)
            place = jnp.where(flag_own > 0.5, place_own, place_far + count_own[:, 0:1])
            place = jnp.where(filled, place, -1.0)
            count = count_own + count_far
            rank_rows.append(place[:, 0:LANES])
            stacked = [jnp.concatenate(split3(p), axis=0) for p in pieces]
            total = jnp.max(count)
            chunk[PART * 2 * USED + c : PART * 2 * USED + c + 1, :] = count
            ready.append((place, stacked, count_own, total))

        def move(t, c):
            place, stacked, count_own, _ = ready[c]
            goal_t = goal + float(t * LANES)
            acc = jnp.zeros((3 * FIELDS, LANES), f32)
            for s in range(slots):
                pick = one_hot(goal_t == place[s : s + 1, :])
                acc = acc + dot(stacked[s], pick, ((1,), (1,)))
            x = acc[0:8, :] + acc[8:16, :] + acc[16:24, :]
            at = tile_row(t, c)
            chunk[at : at + USED, :] = x[0:USED, :]
            if t * LANES < own.shape[1]:
                x = jnp.where(row_of == 7, count_own, x)
                own[c * FIELDS : (c + 1) * FIELDS, t * LANES : (t + 1) * LANES] = x

        for t in range(PART):
            for c in range(2):
                move(t, c)

        @pl.when(jnp.maximum(ready[0][3], ready[1][3]) > PART * LANES)
        def _():
            for t in range(PART, tiles):
                for c in range(2):
                    move(t, c)

        ranks[...] = jnp.transpose(jnp.concatenate(rank_rows + [jnp.zeros((LANES - 2 * slots, LANES), f32)], axis=0))
        value = chunk[0 : part_rows(), :]
        for d in range(members):
            out[d] = value
        rest[...] = chunk[part_rows() :, :]

    return body


def prepare_body(peers, slots):
    used = 2 * USED

    def body(own, ranks, wide, pick):
        own_width = peers * slots
        stacked = jnp.concatenate([p.astype(f32) for p in split3(own[...])], axis=0)
        columns = jnp.transpose(stacked).astype(bf16)
        spread_to = iota((6 * FIELDS, used * LANES), 1) >> 7
        field_of = spread_to + jnp.where(spread_to >= USED, FIELDS - USED, 0)
        spread = one_hot((iota((6 * FIELDS, used * LANES), 0) & (2 * FIELDS - 1)) == field_of)
        wide[...] = dot(columns, spread, ((1,), (0,)))
        goal = iota((peers, own_width), 1).astype(f32)
        for c in range(2):
            for s in range(slots):
                rank = ranks[0:peers, c * slots + s : c * slots + s + 1]
                pick[s * peers : (s + 1) * peers, c * own_width : (c + 1) * own_width] = one_hot(rank == goal)

    return body


def match_body(peers, slots, members, tiles):
    block = 8 * GROUPS
    whole = tiles > PART
    usual = PART
    rows = part_rows()
    own_width = peers * slots
    early = own_width * 3 // 4

    prepare = prepare_body(peers, slots)

    def body(*refs):
        near, refs = refs[: 1 + whole], refs[1 + whole :]
        own, ranks, out, refs = refs[0], refs[1], refs[2], refs[3:]
        over, refs = refs[: 1 - whole], refs[1 - whole :]
        wide, pick, line, totals, values = refs
        prepare(own, ranks, wide, pick)
        lane8 = iota((8, LANES), 1)
        count_own = [jnp.max(own[c * FIELDS + 7 : c * FIELDS + 8, 0:LANES]).astype(i32) for c in range(2)]

        def count_of(d, c):
            at = d * rows + PART * 2 * USED + c
            return jnp.max(near[0][at : at + 1, :]).astype(i32)

        counts = [[count_of(d, c) for d in range(members)] for c in range(2)]
        if not whole:
            most = counts[0][0]
            for n in counts[0][1:] + counts[1]:
                most = jnp.maximum(most, n)
            over[0][0, 0] = (most > PART * LANES).astype(i32)
            counts = [[jnp.minimum(n, PART * LANES) for n in line_counts] for line_counts in counts]
        ends = []
        for c in range(2):
            start = jnp.int32(0)
            for d in range(members):
                shift = start & (LANES - 1)
                base = start >> 7
                keep = lane8 >= shift

                def put(k, x, c=c, base=base):
                    line[c, base + k] = x

                def turned(k, c=c, d=d, shift=shift):
                    at = d * rows + tile_row(k % PART, c)
                    return pltpu.roll(near[k // PART][at : at + FIELDS, :], shift, 1)

                last = jnp.zeros((FIELDS, LANES), f32) if d == 0 else line[c, base]
                for k in range(usual):
                    now = turned(k)
                    put(k, jnp.where(keep, now, last))
                    last = now
                put(usual, jnp.where(keep, 0.0, last))
                put(usual + 1, jnp.zeros((FIELDS, LANES), f32))

                if not whole:
                    start = start + counts[c][d]
                    continue

                @pl.when(counts[c][d] > usual * LANES)
                def _(c=c, base=base, keep=keep, put=put, turned=turned):
                    last = line[c, base + usual]
                    for k in range(usual, tiles):
                        now = turned(k)
                        put(k, jnp.where(keep, now, last))
                        last = now
                    put(tiles, jnp.where(keep, 0.0, last))
                    put(tiles + 1, jnp.zeros((FIELDS, LANES), f32))

                start = start + counts[c][d]
            ends.append(lax.div(start + (2 * LANES - 1), 2 * LANES))

        for c in range(2):
            other = 1 - c
            blocks = lax.div(count_own[c] + (block - 1), block)

            def own_block(b, _, c=c, other=other):
                base = pl.multiple_of(b * block, 8)
                fields = []
                for g in range(GROUPS):
                    col = [wide[pl.ds(base + 8 * g, 8), (c * USED + f) * LANES : (c * USED + f + 1) * LANES] for f in range(USED)]
                    code = col[5].astype(i32)
                    own_code = code + (NCOL + 1 - EMPTY_BIT)
                    mask = jnp.where(code < ROW_BIT, 256, 512) | (EMPTY_BIT | (NCOL - 1))
                    fields.append((col[0] - 1.0, col[1], col[2], col[3], col[4], own_code, mask))

                def pairs(t, acc):
                    acc = [list(a) for a in acc]
                    for half in range(2):
                        at = line.at[other, 2 * t + half]
                        row = [jnp.broadcast_to(at[f : f + 1, :], (8, LANES)) for f in range(USED)]
                        code = row[5].astype(i32) - EMPTY_BIT
                        for g in range(GROUPS):
                            px, py, xx, yy, xy, own_code, mask = fields[g]
                            step = (own_code - code) & mask
                            dx = step.astype(f32) + (px - row[0])
                            dy = py - row[1]
                            sx, sy, sxy = xx + row[2], yy + row[3], xy + row[4]
                            det = sx * sy - 0.25 * (sxy * sxy)
                            root = lax.rsqrt(det)
                            chi = dy * (sxy * dx - sx * dy) - sy * (dx * dx)
                            like = jnp.exp2(chi * (root * root)) * root
                            like = jnp.where(step <= 2, like, 0.0)
                            acc[g][0] = acc[g][0] + like
                            if c == 0:
                                acc[g][1] = acc[g][1] + like * dx
                                acc[g][2] = acc[g][2] + like * dy
                    return tuple(tuple(a) for a in acc)

                zero = jnp.zeros((8, LANES), f32)
                acc = tuple((zero,) * (3 if c == 0 else 1) for _ in range(GROUPS))
                acc = lax.fori_loop(0, ends[other], pairs, acc)
                for g in range(GROUPS):
                    for k, a in enumerate(acc[g]):
                        totals[3 * c + k, pl.ds(base + 8 * g, 8), :] = a
                return 0

            lax.fori_loop(0, blocks, own_block, 0)

        f_of_lane = lane8 & (SLOT_LANES - 1)

        def sum_rows(first, last):
            for c in range(2):
                for g in range(first // 8, last // 8):
                    live = (iota((8, LANES), 0) + 8 * g) < count_own[c]
                    value = jnp.zeros((8, LANES), f32)
                    for k in range(3 if c == 0 else 1):
                        total = jnp.sum(totals[3 * c + k, 8 * g : 8 * g + 8, :], axis=1, keepdims=True) * GAIN
                        value = jnp.where(f_of_lane == c * FIELDS + k, total, value)
                    values[c * own_width + 8 * g : c * own_width + 8 * g + 8, :] = jnp.where(live, value, 0.0)

        many = jnp.maximum(count_own[0], count_own[1]) > early
        sum_rows(0, early)

        @pl.when(many)
        def _():
            sum_rows(early, own_width)

        @pl.when(jnp.logical_not(many))
        def _():
            for c in range(2):
                values[c * own_width + early : (c + 1) * own_width, :] = jnp.zeros((own_width - early, LANES), f32)

        result = sum(dot(pick[...], part, ((1,), (0,))) for part in split3(values[...])[:2])
        slot_of_lane = iota((peers, LANES), 1) >> 4
        final = jnp.zeros((peers, LANES), f32)
        for s in range(slots):
            final = final + jnp.where(slot_of_lane == s, result[s * peers : (s + 1) * peers, :], 0.0)
        out[...] = final

    return body


def return_body(sub_count, peers):
    slots = CAP * sub_count

    def body(back, places, like, offset, wise):
        n = places.shape[1]
        at = jnp.concatenate([places[0:1, :], places[1:2, :]], axis=1)
        rank_g, rank_w = places[2:3, :], places[3:4, :]
        pick = one_hot(iota((peers, 2 * n), 0) == at)
        turned = jnp.transpose(back[...])
        found = sum(dot(part, pick, ((1,), (0,))) for part in split3(turned)[:2])
        gaia = jnp.zeros((FIELDS, n), f32)
        other = jnp.zeros((FIELDS, n), f32)
        for s in range(slots):
            at = s * SLOT_LANES
            gaia = gaia + jnp.where(rank_g == s, found[at : at + FIELDS, 0:n], 0.0)
            other = other + jnp.where(rank_w == s, found[at + FIELDS : at + 2 * FIELDS, n : 2 * n], 0.0)
        like[...] = gaia[0:1, :]
        offset[...] = gaia[1:3, :]
        wise[...] = other[0:1, :]

    return body


def stages(pix_count, sub_count, rep_count, n):
    peers = pix_count
    members = sub_count * rep_count
    slots = CAP * sub_count
    width = 3 * peers * slots
    own_width = peers * slots
    rows = part_rows()
    parts = width // LANES // PART
    pair, line, whole = pltpu.VMEM((2, n), f32), pltpu.VMEM((1, n), f32), pltpu.VMEM((1, n), i32)
    send = call(
        send_body(pix_count, sub_count, peers),
        (jax.ShapeDtypeStruct((3 * peers, LANES), f32), jax.ShapeDtypeStruct((8, n), i32)),
    )
    compact = call(
        compact_body(peers, slots, members, width),
        (
            jax.ShapeDtypeStruct((members, rows, LANES), f32),
            jax.ShapeDtypeStruct(((parts - 1) * rows, LANES), f32),
            jax.ShapeDtypeStruct((2 * FIELDS, own_width), f32),
            jax.ShapeDtypeStruct((LANES, LANES), f32),
        ),
        [pltpu.VMEM((parts * rows, LANES), f32)],
    )
    results = jax.ShapeDtypeStruct((peers, LANES), f32)
    held = lambda tiles: [
        pltpu.VMEM((own_width, 2 * USED * LANES), f32),
        pltpu.VMEM((own_width, 2 * own_width), bf16),
        pltpu.VMEM((2, members * tiles + 8, FIELDS, LANES), f32),
        pltpu.VMEM((4, own_width, LANES), f32),
        pltpu.VMEM((2 * own_width, LANES), f32),
    ]
    match = call(
        match_body(peers, slots, members, PART),
        (results, jax.ShapeDtypeStruct((1, 1), i32)),
        held(PART),
        out_specs=(pl.BlockSpec(memory_space=pltpu.VMEM), pl.BlockSpec(memory_space=pltpu.SMEM)),
    )
    match_whole = call(match_body(peers, slots, members, width // LANES), results, held(width // LANES))
    back = call(
        return_body(sub_count, peers),
        (
            jax.ShapeDtypeStruct((1, n), f32),
            jax.ShapeDtypeStruct((2, n), f32),
            jax.ShapeDtypeStruct((1, n), f32),
        ),
    )
    return send, compact, match, match_whole, back


def shards(gaia_pos, gaia_shape, gaia_corr, gaia_dest, gaia_cell, wise_pos, wise_shape, wise_corr, wise_dest, wise_cell):
    pix_count = lax.axis_size("pix")
    sub_count = lax.axis_size("sub")
    rep_count = lax.axis_size("rep")
    peers = pix_count
    members = sub_count * rep_count
    n = gaia_pos.shape[1]
    send, compact, match, match_whole, back = stages(pix_count, sub_count, rep_count, n)
    row = lambda x: x.reshape(1, n)
    gd, wd = row(gaia_dest), row(wise_dest)
    msg, places = send(gaia_pos, gaia_shape, row(gaia_corr), gd, row(gaia_cell), wise_pos, wise_shape, row(wise_corr), wd, row(wise_cell))
    ring = [[(i + ring_start(pix_count)) % pix_count for i in range(pix_count)]]
    exchange = lambda x: lax.all_to_all(x, "pix", 0, 0, axis_index_groups=ring, tiled=True)
    got = exchange(msg.reshape(peers, 1, 3 * LANES))
    chunks, rest, own, ranks = compact(got.reshape(3 * peers, LANES))
    gather = lambda x: lax.all_to_all(x, ("rep", "sub"), 0, 0, tiled=True).reshape(-1, LANES)
    near = gather(chunks)
    results, over = match(near, own, ranks)

    def with_rest():
        return match_whole(near, gather(jnp.broadcast_to(rest[None], (members, *rest.shape))), own, ranks)

    results = lax.cond(over[0, 0] > 0, with_rest, lambda: results)
    returned = exchange(results.reshape(peers, 1, LANES))
    like, offset, wise = back(returned.reshape(peers, LANES), places)
    return like.reshape(n), offset, wise.reshape(n)


def solution(mesh):
    flat = P(("groups", "pix", "sub", "rep"))
    pair = P(None, ("groups", "pix", "sub", "rep"))
    column = P(("groups", "pix", "sub", "rep"), None)
    return jax.shard_map(
        shards,
        mesh=mesh,
        in_specs=(pair, pair, flat, column, flat, pair, pair, flat, column, flat),
        out_specs=(flat, pair, flat),
        check_vma=False,
    )
```
